128 devices in a mesh: seq: 32 (over z, y, x_hi), dp: 4 (over x_lo, core).
Axes of the slice: x: 4 (x_hi: 2, x_lo: 2; x = x_hi * 2 + x_lo), y: 4, z: 4, core: 2. Of those that a mesh axis runs over, the one named last changes fastest.
Arguments:
- hidden: bfloat16 [4, 8192, 4608], P('dp', 'seq'), may hold values from -6 to 6
- queries: bfloat16 [4, 8192, 2048], P('dp', 'seq'), may hold values from -64 to 64
- down_weight: bfloat16 [4608, 1024], P('dp'), may hold values from -0.09375 to 0.09375
- up_weight: bfloat16 [2, 512, 1024], P(None, 'dp'), may hold values from -0.25 to 0.25
- lengths: int32 [4], P('dp'), may hold values from 2048 to 8192
Outputs:
- latent_cache: bfloat16 [4, 8192, 1024], P('dp', 'seq')
- attended: bfloat16 [4, 8192, 2048], P('dp', 'seq')
The draws below stay inside these ranges and needn't reach their ends.
All inputs are finite; a program needn't handle non-finite values.
Results may differ from the reference program's by a relative error of at most 0.012.
The reference program's roundings to bfloat16 on the way count: a program that leaves them out, or rounds other values in their place, can miss the bound.
Values may be sent and summed in bfloat16 or wider, within the bound.
No kernel may reach another device: no remote copies, remote signals or barrier semaphores. Data moves between devices by JAX's collectives and lax.ppermute only.
A program may use at most 128 MiB of HBM per device.

```python
import math
import jax
import jax.numpy as jnp
from jax import lax

D = 4608
HEAD = 128
Q_HEADS = 16
KV_HEADS = 8
RANK = 1024
WINDOW = 4096
SEQ = 8192
BATCH = 4


def draw_queries(key, part):
    base_key = jax.random.fold_in(key, 11)
    entry_key, scale_key = jax.random.split(base_key)
    entries = jnp.clip(jax.random.normal(entry_key, (BATCH, SEQ, Q_HEADS, HEAD), jnp.float32), -4.0, 4.0)
    lowest, highest = (0.5, 16.0)
    log_scales = jax.random.uniform(scale_key, (BATCH, SEQ, Q_HEADS, 1), jnp.float32, math.log(lowest), math.log(highest))
    scaled = entries * jnp.exp(log_scales)
    return scaled.reshape(BATCH, SEQ, Q_HEADS * HEAD).astype(jnp.bfloat16)


def plant(drawn, stream_key, low, largest):
    extent = drawn.shape
    place = [jax.random.randint(jax.random.fold_in(stream_key, axis), (), 0, extent[axis]) for axis in range(len(extent))]
    drawn = drawn.at[tuple(place)].set(low)
    longest = extent.index(max(extent))
    place[longest] = (place[longest] + 1) % extent[longest]
    return drawn.at[tuple(place)].set(largest)


def block_levels(stream_key, extent, pieces, least, high):
    gain, own = 1.0, jax.random.fold_in(stream_key, 6)
    for dim, parts in pieces:
        steps = jnp.exp(jax.random.uniform(jax.random.fold_in(own, dim), (parts,), jnp.float32, least / len(pieces), high / len(pieces)))
        gain = gain * jnp.repeat(steps, extent[dim] // parts).reshape([-1 if axis == dim else 1 for axis in range(len(extent))])
    return gain


def bell_draw(rng, shape, scale, bound, pieces=(), kind=jnp.bfloat16):
    values = jax.random.normal(rng, shape, jnp.float32) * scale
    if len(pieces) > 0:
        values = block_levels(rng, shape, pieces, -0.22, 0.18) * values
    return jnp.clip(values, min=-bound, max=bound).astype(kind)


def setup_inputs(seed: int = 0) -> dict:
    arg_keys = jax.random.split(jax.random.key(seed), 6)
    return {
        "hidden": bell_draw(arg_keys[0], (BATCH, SEQ, D), 1.0, 6.0, ((0, 4), (1, 32))),
        "queries": draw_queries(jax.random.fold_in(arg_keys[5], 71), 0),
        "down_weight": bell_draw(arg_keys[2], (D, RANK), D ** -0.5, 0.09375, ((0, 4),)),
        "up_weight": bell_draw(arg_keys[3], (2, RANK // 2, KV_HEADS * HEAD), (RANK // 2) ** -0.5, 0.25, ((1, 4),)),
        "lengths": plant(jax.random.randint(arg_keys[4], (BATCH,), SEQ // 4, SEQ + 1), jax.random.fold_in(arg_keys[4], 1), SEQ // 4, SEQ).astype(jnp.int32),
    }


query_scale = 144.0 ** -0.5
soft_cap = 50.0


def rotate(values_in, start_pos):
    batches, count, width = values_in.shape
    half_head = HEAD // 2
    places = (start_pos + jnp.arange(count, dtype=jnp.int32)).astype(jnp.float32)
    freqs = 10000.0 ** (-2.0 * jnp.arange(half_head, dtype=jnp.float32) / HEAD)
    angles = places[:, None] * freqs[None, :]
    cosine = jnp.cos(angles)[None, :, None, :]
    sine_val = jnp.sin(angles)[None, :, None, :]
    split_heads = values_in.reshape(batches, count, width // HEAD, 2, half_head)
    lower = split_heads[:, :, :, 0, :]
    upper = split_heads[:, :, :, 1, :]
    turned = jnp.stack([lower * cosine - upper * sine_val, upper * cosine + lower * sine_val], axis=3)
    return turned.reshape(batches, count, width)


def reference(hidden, queries, down_weight, up_weight, lengths):
    flat_hidden = hidden.reshape(BATCH * SEQ, D)
    latent = jnp.dot(flat_hidden, down_weight, preferred_element_type=jnp.float32).astype(jnp.bfloat16)
    latent = latent.reshape(BATCH, SEQ, RANK)
    positions = jnp.arange(SEQ, dtype=jnp.int32)
    is_live = positions[None, :] < lengths[:, None]
    latent = jnp.where(is_live[:, :, None], latent, jnp.zeros((), jnp.bfloat16))
    key_rank = RANK // 2
    kv_width = KV_HEADS * HEAD
    keys_raw = jnp.dot(latent[:, :, :key_rank].reshape(-1, key_rank), up_weight[0], preferred_element_type=jnp.float32)
    keys_all = rotate(keys_raw.reshape(BATCH, SEQ, kv_width), 0).astype(jnp.bfloat16)
    values_all = jnp.dot(latent[:, :, key_rank:].reshape(-1, key_rank), up_weight[1], preferred_element_type=jnp.float32)
    values_all = values_all.astype(jnp.bfloat16).reshape(BATCH, SEQ, kv_width)
    block_rows = math.gcd(512, SEQ)
    blocks = SEQ // block_rows
    padding = jnp.zeros((BATCH, WINDOW, kv_width), jnp.bfloat16)
    keys_pad = jnp.concatenate([padding, keys_all], axis=1)
    values_pad = jnp.concatenate([padding, values_all], axis=1)
    query_width = Q_HEADS * HEAD
    ratio = Q_HEADS // KV_HEADS

    def one_block(flat_index):
        batch_index = (flat_index // blocks).astype(jnp.int32)
        row_start = ((flat_index % blocks) * block_rows).astype(jnp.int32)
        zero_idx = jnp.zeros((), jnp.int32)
        keys_win = lax.dynamic_slice(keys_pad, (batch_index, row_start, zero_idx), (1, WINDOW + block_rows, kv_width))[0]
        values_win = lax.dynamic_slice(values_pad, (batch_index, row_start, zero_idx), (1, WINDOW + block_rows, kv_width))[0]
        query_blk = lax.dynamic_slice(queries, (batch_index, row_start, zero_idx), (1, block_rows, query_width))[0]
        q_split = query_blk.astype(jnp.float32).reshape(block_rows, KV_HEADS, ratio, HEAD)
        keys_grp = keys_win.astype(jnp.float32).reshape(-1, KV_HEADS, HEAD)
        values_grp = values_win.astype(jnp.float32).reshape(-1, KV_HEADS, HEAD)
        raw = jnp.einsum("lgrd,ngd->grln", q_split, keys_grp, precision=lax.Precision.HIGHEST)
        capped = soft_cap * jnp.tanh(raw * (query_scale / soft_cap))
        q_pos = row_start + jnp.arange(block_rows, dtype=jnp.int32)
        key_pos = row_start - WINDOW + jnp.arange(WINDOW + block_rows, dtype=jnp.int32)
        allowed = (key_pos[None, :] <= q_pos[:, None]) & (key_pos[None, :] > q_pos[:, None] - WINDOW) & (key_pos[None, :] >= 0)
        expo = jnp.where(allowed, jnp.exp(capped), 0.0)
        denom = jnp.sum(expo, axis=-1)
        probs = expo.astype(jnp.bfloat16).astype(jnp.float32)
        numer = jnp.einsum("grln,ngd->lgrd", probs, values_grp, precision=lax.Precision.HIGHEST)
        result = numer / jnp.transpose(denom, (2, 0, 1))[..., None]
        result = result.reshape(block_rows, query_width)
        live_rows = q_pos < lengths[batch_index]
        return jnp.where(live_rows[:, None], result, 0.0).astype(jnp.bfloat16)

    outputs = lax.map(one_block, jnp.arange(BATCH * blocks, dtype=jnp.int32))
    attended = outputs.reshape(BATCH, SEQ, query_width)
    return latent, attended
```

```python
import itertools

import jax
import jax.numpy as jnp
from jax import lax
from jax.experimental import pallas as pl
from jax.experimental.pallas import tpu as pltpu
from jax.sharding import Mesh
from jax.sharding import PartitionSpec as P

HEAD = 128
PAIR = 2 * HEAD
BLOCK = 256
CHUNK = 2048
WINDOW = 4096
SIZES = {"z": 4, "y": 4, "xh": 2, "xl": 2, "core": 2}
SEQ_AXES = ("z", "y", "xh")
DP_AXES = ("xl", "core")
PLANE = ("y", "xh")

query_scale = 144.0 ** (-0.5)
soft_cap = 50.0
LOG2E = 1.4426950408889634
CONTRACT_LAST = (((1,), (1,)), ((), ()))


def x_shift(step):
    pairs = []
    for hi, lo in itertools.product(range(2), range(2)):
        to = (2 * hi + lo + step) % 4
        pairs.append((2 * hi + lo, to))
    return pairs


def to_partner(array):
    return lax.ppermute(array, "core", [(0, 1), (1, 0)])


def half_product_kernel(info, own_hidden, partner_hidden, own_weight, partner_weight, out):
    out[...] = jnp.dot(
        own_hidden[...], own_weight[...], preferred_element_type=jnp.float32
    ) + jnp.dot(partner_hidden[...], partner_weight[...], preferred_element_type=jnp.float32)


def project_kernel(
    info, partial, near_hidden, far_hidden, near_left, near_right, far_left, far_right,
    up_own, up_partner, near_keys, near_values, far_keys, far_values, cosine, sine,
    latent, pairs, uppers,
):
    mine, start, length = info[0], info[1], info[2]
    rows = partial.shape[0]
    rank = partial.shape[1] // 2
    piece = up_own.shape[1]
    live = (start + lax.broadcasted_iota(jnp.int32, (rows, rank), 0)) < length

    def place(which, shard, value):
        uppers[which, pl.ds(pl.multiple_of(shard * piece, piece), piece), :] = value

    for which, near, far in ((0, near_keys, far_keys), (1, near_values, far_values)):
        place(which, mine, up_own[which])
        place(which, mine ^ 1, up_partner[which])
        place(which, mine ^ 2, near[...])
        place(which, mine ^ 3, far[...])
    for which, near, far in ((0, near_left, far_left), (1, near_right, far_right)):
        total = (
            partial[:, which * rank : (which + 1) * rank]
            + jnp.dot(near_hidden[...], near[...], preferred_element_type=jnp.float32)
            + jnp.dot(far_hidden[...], far[...], preferred_element_type=jnp.float32)
        )
        rounded = jnp.where(live, total, 0.0).astype(jnp.bfloat16)
        latent[:, which * rank : (which + 1) * rank] = rounded
        raw = jnp.dot(rounded, uppers[which], preferred_element_type=jnp.float32)
        for head in range(raw.shape[1] // HEAD):
            entry = raw[:, head * HEAD : (head + 1) * HEAD]
            if which == 0:
                entry = entry * cosine[...] + pltpu.roll(entry, HEAD // 2, 1) * sine[...]
            pairs[head, :, which * HEAD : (which + 1) * HEAD] = entry.astype(jnp.bfloat16)


def expo(raw):
    return jnp.exp2(jnp.tanh(raw * (query_scale / soft_cap)) * (soft_cap * LOG2E))


def attend_kernel(info, queries, far_pairs, near_pairs, own_pairs, out, pairs, sems):
    plane = info[0]
    copies = [
        pltpu.make_async_copy(ref, pairs.at[pl.ds(CHUNK * i, CHUNK)], sems.at[i])
        for i, ref in enumerate((far_pairs, near_pairs, own_pairs))
    ]
    for copy in copies:
        copy.start()
    for copy in copies:
        copy.wait()
    row = lax.broadcasted_iota(jnp.int32, (2 * BLOCK, BLOCK), 0) % BLOCK
    col = lax.broadcasted_iota(jnp.int32, (2 * BLOCK, BLOCK), 1)
    causal = col <= row
    span = WINDOW // BLOCK

    def folded(values):
        total = values[:, :HEAD]
        for t in range(1, values.shape[1] // HEAD):
            total = total + values[:, t * HEAD : (t + 1) * HEAD]
        return total

    def block(i, carry):
        index = (CHUNK // BLOCK) * plane + i
        base = pl.multiple_of(i * BLOCK, BLOCK)
        own = queries[pl.ds(base, BLOCK), :]
        stacked = jnp.concatenate([own[:, :HEAD], own[:, HEAD:]], axis=0)
        diagonal = pl.multiple_of(base + WINDOW, BLOCK)

        def score(offset):
            keys = pairs[pl.ds(offset, BLOCK), :HEAD]
            return lax.dot_general(
                stacked, keys, CONTRACT_LAST, preferred_element_type=jnp.float32
            )

        def weighted(probs, offset):
            return jnp.dot(
                probs.astype(jnp.bfloat16),
                pairs[pl.ds(offset, BLOCK), HEAD:],
                preferred_element_type=jnp.float32,
            )

        def finish(numer, denom):
            result = numer / jnp.sum(denom, axis=1, keepdims=True)
            out[pl.ds(base, BLOCK), :] = jnp.concatenate(
                [result[:BLOCK], result[BLOCK:]], axis=1
            ).astype(out.dtype)

        @pl.when(index >= span)
        def _():
            e = expo(jnp.where(causal, score(diagonal), score(base)))
            denom = folded(e)
            numer = weighted(jnp.where(causal, e, 0.0), diagonal)
            numer = numer + weighted(jnp.where(causal, 0.0, e), base)
            for t in range(1, span):
                offset = pl.multiple_of(base + t * BLOCK, BLOCK)
                e = expo(score(offset))
                denom = denom + folded(e)
                numer = numer + weighted(e, offset)
            finish(numer, denom)

        @pl.when(index < span)
        def _():
            e = jnp.where(causal, expo(score(diagonal)), 0.0)
            denom = folded(e)
            numer = weighted(e, diagonal)
            first = WINDOW - plane * CHUNK

            def step(t, state):
                numer, denom = state
                for u in range(4):
                    offset = pl.multiple_of(first + (t * 4 + u) * BLOCK, BLOCK)
                    e = jnp.where(t * 4 + u < index, expo(score(offset)), 0.0)
                    denom = denom + folded(e)
                    numer = numer + weighted(e, offset)
                return numer, denom

            finish(*lax.fori_loop(0, (index + 3) // 4, step, (numer, denom)))

        return carry

    lax.fori_loop(0, CHUNK // BLOCK, block, 0)


def body(hidden, queries, down_weight, up_weight, lengths):
    _, rows, width = hidden.shape
    rank2 = down_weight.shape[1]
    rank = rank2 // 2
    depth = down_weight.shape[0]
    kv_width = up_weight.shape[2]
    groups = kv_width // HEAD
    hidden = hidden[0]
    mine = 2 * lax.axis_index("xl") + lax.axis_index("core")
    plane = lax.axis_index("z")
    seq_index = lax.axis_index(SEQ_AXES)
    start = seq_index * rows
    info = jnp.stack([mine, start, lengths[0]]).astype(jnp.int32)

    forward, backward = x_shift(1), x_shift(-1)
    near_left = lax.ppermute(down_weight[:, :rank], ("xh", "xl"), forward)
    near_right = lax.ppermute(down_weight[:, rank:], ("xh", "xl"), backward)
    near_keys = lax.ppermute(up_weight[0], ("xh", "xl"), forward)
    near_values = lax.ppermute(up_weight[1], ("xh", "xl"), backward)
    partner_weight = to_partner(down_weight)
    up_partner = to_partner(up_weight)
    far_left, far_right = to_partner(near_left), to_partner(near_right)
    far_keys, far_values = to_partner(near_keys), to_partner(near_values)

    sent = queries[0].reshape(rows, groups, PAIR).transpose(1, 0, 2)
    my_queries = lax.all_to_all(sent, PLANE, 0, 0, tiled=True).reshape(CHUNK, PAIR)

    half = HEAD // 2
    places = (start + jnp.arange(rows, dtype=jnp.int32)).astype(jnp.float32)
    freqs = 10000.0 ** (-2.0 * jnp.arange(half, dtype=jnp.float32) / HEAD)
    angles = places[:, None] * freqs[None, :]
    cosine, sine = jnp.cos(angles), jnp.sin(angles)
    cosine = jnp.concatenate([cosine, cosine], axis=1)
    sine = jnp.concatenate([-sine, sine], axis=1)

    def hidden_part(flip):
        return pl.BlockSpec((rows, depth), lambda i, s: (0, s[0] ^ flip))

    def whole(shape):
        return pl.BlockSpec(shape, lambda i, s: (0,) * len(shape))

    partial = pl.pallas_call(
        half_product_kernel,
        out_shape=jax.ShapeDtypeStruct((rows, rank2), jnp.float32),
        grid_spec=pltpu.PrefetchScalarGridSpec(
            num_scalar_prefetch=1,
            grid=(1,),
            in_specs=[hidden_part(0), hidden_part(1)] + [whole((depth, rank2))] * 2,
            out_specs=whole((rows, rank2)),
        ),
        compiler_params=pltpu.CompilerParams(vmem_limit_bytes=40 * 2**20),
        cost_estimate=pl.CostEstimate(
            flops=4 * rows * depth * rank2, bytes_accessed=8 * 2**20, transcendentals=0
        ),
        name="half_product",
    )(info, hidden, hidden, down_weight, partner_weight)

    piece = up_weight.shape[1]
    latent, pairs = pl.pallas_call(
        project_kernel,
        out_shape=(
            jax.ShapeDtypeStruct((rows, rank2), jnp.bfloat16),
            jax.ShapeDtypeStruct((groups, rows, PAIR), jnp.bfloat16),
        ),
        grid_spec=pltpu.PrefetchScalarGridSpec(
            num_scalar_prefetch=1,
            grid=(1,),
            in_specs=[whole((rows, rank2)), hidden_part(2), hidden_part(3)]
            + [whole((depth, rank))] * 4
            + [whole((2, piece, kv_width))] * 2
            + [whole((piece, kv_width))] * 4
            + [whole((rows, HEAD))] * 2,
            out_specs=[whole((rows, rank2)), whole((groups, rows, PAIR))],
            scratch_shapes=[pltpu.VMEM((2, rank, kv_width), jnp.bfloat16)],
        ),
        compiler_params=pltpu.CompilerParams(vmem_limit_bytes=48 * 2**20),
        cost_estimate=pl.CostEstimate(
            flops=4 * rows * depth * rank2, bytes_accessed=10 * 2**20, transcendentals=0
        ),
        name="project",
    )(
        info, partial, hidden, hidden, near_left, near_right, far_left, far_right,
        up_weight, up_partner, near_keys, near_values, far_keys, far_values, cosine, sine,
    )

    own_pairs = lax.all_to_all(pairs, PLANE, 0, 0, tiled=True).reshape(CHUNK, PAIR)
    near_pairs = lax.ppermute(own_pairs, "z", [(0, 1), (1, 2), (2, 3)])
    far_pairs = lax.ppermute(own_pairs, "z", [(0, 2), (1, 3)])

    anywhere = pl.BlockSpec(memory_space=pl.ANY)
    result = pl.pallas_call(
        attend_kernel,
        out_shape=jax.ShapeDtypeStruct((CHUNK, PAIR), jnp.bfloat16),
        in_specs=[
            pl.BlockSpec(memory_space=pltpu.SMEM),
            pl.BlockSpec(memory_space=pltpu.VMEM),
            anywhere,
            anywhere,
            anywhere,
        ],
        out_specs=pl.BlockSpec(memory_space=pltpu.VMEM),
        scratch_shapes=[
            pltpu.VMEM((WINDOW + CHUNK, PAIR), jnp.bfloat16),
            pltpu.SemaphoreType.DMA((3,)),
        ],
        compiler_params=pltpu.CompilerParams(vmem_limit_bytes=48 * 2**20),
        cost_estimate=pl.CostEstimate(
            flops=10**10, bytes_accessed=5 * 2**20, transcendentals=3 * 10**7
        ),
        name="attend",
    )(plane.reshape(1).astype(jnp.int32), my_queries, far_pairs, near_pairs, own_pairs)

    home = lax.all_to_all(result.reshape(groups, rows, PAIR), PLANE, 0, 0, tiled=True)
    home = home.transpose(1, 0, 2).reshape(rows, groups * PAIR)
    live = (start + jnp.arange(rows, dtype=jnp.int32)) < lengths[0]
    attended = jnp.where(live[:, None], home, jnp.zeros((), jnp.bfloat16))
    return latent[None], attended[None]


def solution(mesh):
    split = Mesh(mesh.devices.reshape(tuple(SIZES.values())), tuple(SIZES))
    rows = P(DP_AXES, SEQ_AXES, None)
    placed = (rows, rows, P(DP_AXES, None), P(None, DP_AXES, None), P(DP_AXES))
    return jax.shard_map(
        body, mesh=split, in_specs=placed, out_specs=(rows, rows), check_vma=False
    )
```

```python
import functools
import itertools

import jax
import jax.numpy as jnp
from jax import lax
from jax.experimental import pallas as pl
from jax.experimental.pallas import tpu as pltpu
from jax.sharding import Mesh
from jax.sharding import PartitionSpec as P


HEAD = 128
PAIR = 2 * HEAD
BLOCK = 256
CHUNK = 2048
BLOCKS = CHUNK // BLOCK
LOW, MIDDLE = 3, 6
SIZES = {"z": 4, "y": 4, "xh": 2, "xl": 2, "core": 2}
SEQ_AXES = ("z", "y", "xh")
DP_AXES = ("xl", "core")
PLANE = ("y", "xh")

query_scale = 144.0 ** (-0.5)
soft_cap = 50.0
LOG2E = 1.4426950408889634
CONTRACT_LAST = (((1,), (1,)), ((), ()))


def x_shift(step):
    pairs = []
    for hi, lo in itertools.product(range(2), range(2)):
        to = (2 * hi + lo + step) % 4
        pairs.append((2 * hi + lo, to))
    return pairs


def to_partner(array):
    return lax.ppermute(array, "core", [(0, 1), (1, 0)])


def half_product_kernel(info, own_hidden, partner_hidden, own_weight, partner_weight, out):
    out[...] = jnp.dot(
        own_hidden[...], own_weight[...], preferred_element_type=jnp.float32
    ) + jnp.dot(partner_hidden[...], partner_weight[...], preferred_element_type=jnp.float32)


def project_kernel(
    info, partial, near_hidden, far_hidden, near_left, near_right, far_left, far_right,
    up_own, up_partner, near_keys, near_values, far_keys, far_values, cosine, sine,
    latent, pairs, uppers,
):
    mine, start, length = info[0], info[1], info[2]
    rows = partial.shape[0]
    rank = partial.shape[1] // 2
    piece = up_own.shape[1]
    live = (start + lax.broadcasted_iota(jnp.int32, (rows, rank), 0)) < length

    def place(which, shard, value):
        uppers[which, pl.ds(pl.multiple_of(shard * piece, piece), piece), :] = value

    for which, near, far in ((0, near_keys, far_keys), (1, near_values, far_values)):
        place(which, mine, up_own[which])
        place(which, mine ^ 1, up_partner[which])
        place(which, mine ^ 2, near[...])
        place(which, mine ^ 3, far[...])
    for which, near, far in ((0, near_left, far_left), (1, near_right, far_right)):
        total = (
            partial[:, which * rank : (which + 1) * rank]
            + jnp.dot(near_hidden[...], near[...], preferred_element_type=jnp.float32)
            + jnp.dot(far_hidden[...], far[...], preferred_element_type=jnp.float32)
        )
        rounded = jnp.where(live, total, 0.0).astype(jnp.bfloat16)
        latent[:, which * rank : (which + 1) * rank] = rounded
        raw = jnp.dot(rounded, uppers[which], preferred_element_type=jnp.float32)
        for head in range(raw.shape[1] // HEAD):
            entry = raw[:, head * HEAD : (head + 1) * HEAD]
            if which == 0:
                entry = entry * cosine[...] + pltpu.roll(entry, HEAD // 2, 1) * sine[...]
            pairs[head, :, which * HEAD : (which + 1) * HEAD] = entry.astype(jnp.bfloat16)


def expo(raw):
    return jnp.exp2(jnp.tanh(raw * (query_scale / soft_cap)) * (soft_cap * LOG2E))


def folded(values):
    total = values[:, :HEAD]
    for t in range(1, values.shape[1] // HEAD):
        total = total + values[:, t * HEAD : (t + 1) * HEAD]
    return total


def triangle(newer):
    row = lax.broadcasted_iota(jnp.int32, (2 * BLOCK, BLOCK), 0) % BLOCK
    col = lax.broadcasted_iota(jnp.int32, (2 * BLOCK, BLOCK), 1)
    return col <= row if newer else col > row


def stacked_rows(queries, i):
    own = queries[pl.ds(pl.multiple_of(i * BLOCK, BLOCK), BLOCK), :]
    return jnp.concatenate([own[:, :HEAD], own[:, HEAD:]], axis=0)


def over_blocks(stacked, pairs, blocks):
    numer = denom = 0.0
    for j, mask in blocks:
        at = pl.ds(j * BLOCK, BLOCK)
        raw = lax.dot_general(
            stacked, pairs[at, :HEAD], CONTRACT_LAST, preferred_element_type=jnp.float32
        )
        e = expo(raw)
        if mask is not None:
            e = jnp.where(mask, e, 0.0)
        denom = denom + folded(e)
        numer = numer + jnp.dot(
            e.astype(jnp.bfloat16), pairs[at, HEAD:], preferred_element_type=jnp.float32
        )
    return numer, denom


def state_rows(i):
    return pl.ds(pl.multiple_of(i * 2 * BLOCK, 2 * BLOCK), 2 * BLOCK)


def own_kernel(queries, pairs, numer, denom):
    mask = triangle(True)
    for i in range(BLOCKS):
        blocks = [(j, None) for j in range(i)] + [(i, mask)]
        numer[state_rows(i), :], denom[state_rows(i), :] = over_blocks(
            stacked_rows(queries, i), pairs, blocks
        )


def near_kernel(group, info, queries, pairs, numer_in, denom_in, numer, denom):
    blocks = [(j, None) for j in range(pairs.shape[0] // BLOCK)]

    @pl.when(info[0] >= 1)
    def _():
        def step(t, carry):
            for u in range(group):
                i = t * group + u
                n, d = over_blocks(stacked_rows(queries, i), pairs, blocks)
                numer[state_rows(i), :] += n
                denom[state_rows(i), :] += d
            return carry

        lax.fori_loop(0, BLOCKS // group, step, 0)


def far_kernel(first, last, info, queries, pairs, numer_in, denom_in, *outs):
    end = first + pairs.shape[0] // BLOCK
    mask = triangle(False)
    numer, denom = (numer_in, denom_in) if last else outs

    def finish(i, n, d):
        if last:
            n = n / jnp.sum(d, axis=1, keepdims=True)
            outs[0][i * BLOCK : (i + 1) * BLOCK, :] = jnp.concatenate(
                [n[:BLOCK], n[BLOCK:]], axis=1
            ).astype(jnp.bfloat16)
        else:
            numer[state_rows(i), :], denom[state_rows(i), :] = n, d

    @pl.when(info[0] >= 2)
    def _():
        for i in range(BLOCKS):
            blocks = [(j - first, mask if j == i else None) for j in range(max(i, first), end)]
            old_n, old_d = numer[state_rows(i), :], denom[state_rows(i), :]
            if blocks:
                n, d = over_blocks(stacked_rows(queries, i), pairs, blocks)
                finish(i, old_n + n, old_d + d)
            elif last:
                finish(i, old_n, old_d)

    if last:

        @pl.when(info[0] < 2)
        def _():
            for i in range(BLOCKS):
                finish(i, numer[state_rows(i), :], denom[state_rows(i), :])


IN_VMEM = pl.BlockSpec(memory_space=pltpu.VMEM)
IN_SMEM = pl.BlockSpec(memory_space=pltpu.SMEM)
STATE = jax.ShapeDtypeStruct((2 * CHUNK, HEAD), jnp.float32)
RESULT = jax.ShapeDtypeStruct((CHUNK, PAIR), jnp.bfloat16)


def attention_call(kernel, count, args, result=False, resume=True):
    single = BLOCK * 2 * BLOCK
    inputs = [IN_SMEM] + [IN_VMEM] * 4 if resume else [IN_VMEM] * 2
    return pl.pallas_call(
        kernel,
        out_shape=RESULT if result else (STATE, STATE),
        in_specs=inputs,
        out_specs=IN_VMEM if result else (IN_VMEM, IN_VMEM),
        input_output_aliases={3: 0, 4: 1} if resume and not result else {},
        compiler_params=pltpu.CompilerParams(vmem_limit_bytes=24 * 2**20),
        cost_estimate=pl.CostEstimate(
            flops=count * single * 4 * HEAD, bytes_accessed=2**22, transcendentals=2 * count * single
        ),
    )(*args)


def body(hidden, queries, down_weight, up_weight, lengths):
    _, rows, _ = hidden.shape
    rank2 = down_weight.shape[1]
    rank = rank2 // 2
    depth = down_weight.shape[0]
    kv_width = up_weight.shape[2]
    groups = kv_width // HEAD
    hidden = hidden[0]
    mine = 2 * lax.axis_index("xl") + lax.axis_index("core")
    plane = lax.axis_index("z")
    seq_index = lax.axis_index(SEQ_AXES)
    start = seq_index * rows
    info = jnp.stack([mine, start, lengths[0]]).astype(jnp.int32)

    forward, backward = x_shift(1), x_shift(-1)
    near_left = lax.ppermute(down_weight[:, :rank], ("xh", "xl"), forward)
    near_right = lax.ppermute(down_weight[:, rank:], ("xh", "xl"), backward)
    near_keys = lax.ppermute(up_weight[0], ("xh", "xl"), forward)
    near_values = lax.ppermute(up_weight[1], ("xh", "xl"), backward)
    partner_weight = to_partner(down_weight)
    up_partner = to_partner(up_weight)
    far_left, far_right = to_partner(near_left), to_partner(near_right)
    far_keys, far_values = to_partner(near_keys), to_partner(near_values)

    sent = queries[0].reshape(rows, groups, PAIR).transpose(1, 0, 2)
    my_queries = lax.all_to_all(sent, PLANE, 0, 0, tiled=True).reshape(CHUNK, PAIR)

    half = HEAD // 2
    places = (start + jnp.arange(rows, dtype=jnp.int32)).astype(jnp.float32)
    freqs = 10000.0 ** (-2.0 * jnp.arange(half, dtype=jnp.float32) / HEAD)
    angles = places[:, None] * freqs[None, :]
    cosine, sine = jnp.cos(angles), jnp.sin(angles)
    cosine = jnp.concatenate([cosine, cosine], axis=1)
    sine = jnp.concatenate([-sine, sine], axis=1)

    info, my_queries = lax.optimization_barrier((info, my_queries))

    def hidden_part(flip):
        return pl.BlockSpec((rows, depth), lambda i, s: (0, s[0] ^ flip))

    def whole(shape):
        return pl.BlockSpec(shape, lambda i, s: (0,) * len(shape))

    partial = pl.pallas_call(
        half_product_kernel,
        out_shape=jax.ShapeDtypeStruct((rows, rank2), jnp.float32),
        grid_spec=pltpu.PrefetchScalarGridSpec(
            num_scalar_prefetch=1,
            grid=(1,),
            in_specs=[hidden_part(0), hidden_part(1)] + [whole((depth, rank2))] * 2,
            out_specs=whole((rows, rank2)),
        ),
        compiler_params=pltpu.CompilerParams(vmem_limit_bytes=40 * 2**20),
        cost_estimate=pl.CostEstimate(
            flops=4 * rows * depth * rank2, bytes_accessed=8 * 2**20, transcendentals=0
        ),
        name="half_product",
    )(info, hidden, hidden, down_weight, partner_weight)

    piece = up_weight.shape[1]
    latent, pairs = pl.pallas_call(
        project_kernel,
        out_shape=(
            jax.ShapeDtypeStruct((rows, rank2), jnp.bfloat16),
            jax.ShapeDtypeStruct((groups, rows, PAIR), jnp.bfloat16),
        ),
        grid_spec=pltpu.PrefetchScalarGridSpec(
            num_scalar_prefetch=1,
            grid=(1,),
            in_specs=[whole((rows, rank2)), hidden_part(2), hidden_part(3)]
            + [whole((depth, rank))] * 4
            + [whole((2, piece, kv_width))] * 2
            + [whole((piece, kv_width))] * 4
            + [whole((rows, HEAD))] * 2,
            out_specs=[whole((rows, rank2)), whole((groups, rows, PAIR))],
            scratch_shapes=[pltpu.VMEM((2, rank, kv_width), jnp.bfloat16)],
        ),
        compiler_params=pltpu.CompilerParams(vmem_limit_bytes=48 * 2**20),
        cost_estimate=pl.CostEstimate(
            flops=4 * rows * depth * rank2, bytes_accessed=10 * 2**20, transcendentals=0
        ),
        name="project",
    )(
        info, partial, hidden, hidden, near_left, near_right, far_left, far_right,
        up_weight, up_partner, near_keys, near_values, far_keys, far_values, cosine, sine,
    )

    own_pairs = lax.all_to_all(pairs, PLANE, 0, 0, tiled=True).reshape(CHUNK, PAIR)
    low, middle = LOW * BLOCK, MIDDLE * BLOCK
    up = [(0, 1), (1, 2), (2, 3)]
    near_low = lax.ppermute(own_pairs[:low], "z", up)
    passing = lax.ppermute(own_pairs[low:], "z", [(1, 0), (0, 3)])
    near_middle = lax.ppermute(own_pairs[low:middle], "z", up)
    near_high = lax.ppermute(own_pairs[middle:], "z", up)
    far_low = lax.ppermute(near_low, "z", [(1, 2), (2, 3)])

    spot = plane.reshape(1).astype(jnp.int32)
    state = attention_call(own_kernel, 36, (my_queries, own_pairs), resume=False)
    for name, piece_pairs in (("low", near_low), ("middle", near_middle), ("high", near_high)):
        state = attention_call(
            functools.partial(near_kernel, 2),
            piece_pairs.shape[0] // BLOCK * BLOCKS,
            (spot, my_queries, piece_pairs, *state),
        )
        if name == "low":
            passing, state = lax.optimization_barrier((passing, state))
            far_high = lax.ppermute(passing, "z", [(0, 3), (3, 2)])
    state = attention_call(
        functools.partial(far_kernel, LOW, False), 30,
        (spot, my_queries, far_high, *state),
    )
    result = attention_call(
        functools.partial(far_kernel, 0, True), 6,
        (spot, my_queries, far_low, *state), result=True,
    )

    home = lax.all_to_all(result.reshape(groups, rows, PAIR), PLANE, 0, 0, tiled=True)
    home = home.transpose(1, 0, 2).reshape(rows, groups * PAIR)
    live = (start + jnp.arange(rows, dtype=jnp.int32)) < lengths[0]
    attended = jnp.where(live[:, None], home, jnp.zeros((), jnp.bfloat16))
    return latent[None], attended[None]


def solution(mesh):
    split = Mesh(mesh.devices.reshape(tuple(SIZES.values())), tuple(SIZES))
    rows = P(DP_AXES, SEQ_AXES, None)
    placed = (rows, rows, P(DP_AXES, None), P(None, DP_AXES, None), P(DP_AXES))

    return jax.shard_map(body, mesh=split, in_specs=placed, out_specs=(rows, rows), check_vma=False)
```

```python
import functools
import itertools

import jax
import jax.numpy as jnp
from jax import lax
from jax.experimental import pallas as pl
from jax.experimental.pallas import tpu as pltpu
from jax.sharding import Mesh
from jax.sharding import PartitionSpec as P


HEAD = 128
PAIR = 2 * HEAD
BLOCK = 256
CHUNK = 2048
BLOCKS = CHUNK // BLOCK
LOW, MIDDLE = 3, 6
RELAYED = 704
SIZES = {"z": 4, "y": 4, "xh": 2, "xl": 2, "core": 2}
SEQ_AXES = ("z", "y", "xh")
DP_AXES = ("xl", "core")
PLANE = ("y", "xh")

query_scale = 144.0 ** (-0.5)
soft_cap = 50.0
LOG2E = 1.4426950408889634
CONTRACT_LAST = (((1,), (1,)), ((), ()))


X_AXES = ("xh", "xl", "core")


def x_step(flip):
    pairs = []
    for x, core in itertools.product(range(4), range(2)):
        to = (x + (1 if core == 0 else -1)) % 4
        pairs.append((2 * x + core, 2 * to + (core ^ flip)))
    return pairs


def ring(step):
    return [(i, (i + step) % 4) for i in range(4)]


def to_partner(array):
    return lax.ppermute(array, "core", [(0, 1), (1, 0)])


def both_sequences(own, partner, weight):
    stacked = jnp.concatenate([own, partner], axis=0)
    return jnp.dot(stacked, weight, preferred_element_type=jnp.float32)


def half_product_kernel(info, own_0, own_1, partner_0, partner_1, weight_0, weight_1, out):
    out[...] = both_sequences(own_0[...], partner_0[...], weight_0[...]) + both_sequences(
        own_1[...], partner_1[...], weight_1[...]
    )


def project_kernel(
    info, partial, own_2, own_3, partner_2, partner_3, direct_a, direct_b,
    relay_0, relay_1, relay_2, relay_3, up_own, up_partner, cosine, sine,
    latent, pairs, weights, upper,
):
    mine, plane = info[0], info[1]
    core = mine % 2
    rows = own_2.shape[0]
    piece = up_own.shape[1]
    share = relay_0.shape[1]
    half = direct_a.shape[1]
    split = direct_a.shape[0] - 2 * piece
    for which, direct in ((0, direct_a), (1, direct_b)):
        weights[which, :split, :] = direct[:split, :]
        for step, relay in ((0, relay_0), (3, relay_1), (1, relay_2), (2, relay_3)):
            at = split + share * ((plane + step) % 4)
            weights[which, pl.ds(pl.multiple_of(at, 16), share), :] = relay[which]
        at = pl.ds(pl.multiple_of((mine ^ (2 + which)) * piece, piece), piece)
        upper[at, :half] = direct[split : split + piece, :]
        upper[at, half:] = direct[split + piece :, :]
    upper[pl.ds(pl.multiple_of(mine * piece, piece), piece), :] = up_own[0]
    upper[pl.ds(pl.multiple_of((mine ^ 1) * piece, piece), piece), :] = up_partner[0]
    total = partial[...] + both_sequences(own_2[...], partner_2[...], weights[0])
    total = total + both_sequences(own_3[...], partner_3[...], weights[1])
    rounded = total.astype(jnp.bfloat16)
    latent[...] = rounded
    raw = jnp.dot(rounded, upper[...], preferred_element_type=jnp.float32)
    for which, turn in ((0, core), (1, 1 - core)):
        for head in range(raw.shape[1] // HEAD):
            entry = raw[which * rows : (which + 1) * rows, head * HEAD : (head + 1) * HEAD]
            entry = entry * cosine[...] + pltpu.roll(entry, HEAD // 2, 1) * sine[...]
            pairs[2 * head + turn] = entry.astype(jnp.bfloat16)


def expo(raw):
    return jnp.exp2(jnp.tanh(raw * (query_scale / soft_cap)) * (soft_cap * LOG2E))


def folded(values):
    total = values[:, :HEAD]
    for t in range(1, values.shape[1] // HEAD):
        total = total + values[:, t * HEAD : (t + 1) * HEAD]
    return total


def triangle(newer):
    row = lax.broadcasted_iota(jnp.int32, (2 * BLOCK, BLOCK), 0) % BLOCK
    col = lax.broadcasted_iota(jnp.int32, (2 * BLOCK, BLOCK), 1)
    return col <= row if newer else col > row


def stacked_rows(queries, i):
    own = queries[pl.ds(pl.multiple_of(i * BLOCK, BLOCK), BLOCK), :]
    return jnp.concatenate([own[:, :HEAD], own[:, HEAD:]], axis=0)


def over_blocks(stacked, pairs, blocks):
    numer = denom = 0.0
    for j, mask in blocks:
        raw = lax.dot_general(
            stacked, pairs[2 * j], CONTRACT_LAST, preferred_element_type=jnp.float32
        )
        e = expo(raw)
        if mask is not None:
            e = jnp.where(mask, e, 0.0)
        denom = denom + folded(e)
        numer = numer + jnp.dot(
            e.astype(jnp.bfloat16), pairs[2 * j + 1], preferred_element_type=jnp.float32
        )
    return numer, denom


def state_rows(i):
    return pl.ds(pl.multiple_of(i * 2 * BLOCK, 2 * BLOCK), 2 * BLOCK)


def own_kernel(queries, pairs, numer, denom):
    mask = triangle(True)
    for i in range(BLOCKS):
        blocks = [(j, None) for j in range(i)] + [(i, mask)]
        numer[state_rows(i), :], denom[state_rows(i), :] = over_blocks(
            stacked_rows(queries, i), pairs, blocks
        )


def near_kernel(group, info, queries, pairs, numer_in, denom_in, numer, denom):
    blocks = [(j, None) for j in range(pairs.shape[0] // 2)]

    @pl.when(info[0] >= 1)
    def _():
        def step(t, carry):
            for u in range(group):
                i = t * group + u
                n, d = over_blocks(stacked_rows(queries, i), pairs, blocks)
                numer[state_rows(i), :] += n
                denom[state_rows(i), :] += d
            return carry

        lax.fori_loop(0, BLOCKS // group, step, 0)


def far_kernel(first, last, info, queries, pairs, numer_in, denom_in, *outs):
    end = first + pairs.shape[0] // 2
    mask = triangle(False)
    numer, denom = (numer_in, denom_in) if last else outs

    def finish(i, n, d):
        if last:
            n = n / jnp.sum(d, axis=1, keepdims=True)
            outs[0][i * BLOCK : (i + 1) * BLOCK, :] = jnp.concatenate(
                [n[:BLOCK], n[BLOCK:]], axis=1
            ).astype(jnp.bfloat16)
        else:
            numer[state_rows(i), :], denom[state_rows(i), :] = n, d

    @pl.when(info[0] >= 2)
    def _():
        for i in range(BLOCKS):
            blocks = [(j - first, mask if j == i else None) for j in range(max(i, first), end)]
            old_n, old_d = numer[state_rows(i), :], denom[state_rows(i), :]
            if blocks:
                n, d = over_blocks(stacked_rows(queries, i), pairs, blocks)
                finish(i, old_n + n, old_d + d)
            elif last:
                finish(i, old_n, old_d)

    if last:

        @pl.when(info[0] < 2)
        def _():
            for i in range(BLOCKS):
                finish(i, numer[state_rows(i), :], denom[state_rows(i), :])


IN_VMEM = pl.BlockSpec(memory_space=pltpu.VMEM)
IN_SMEM = pl.BlockSpec(memory_space=pltpu.SMEM)
STATE = jax.ShapeDtypeStruct((2 * CHUNK, HEAD), jnp.float32)
RESULT = jax.ShapeDtypeStruct((CHUNK, PAIR), jnp.bfloat16)


def attention_call(kernel, count, args, result=False, resume=True):
    single = BLOCK * 2 * BLOCK
    inputs = [IN_SMEM] + [IN_VMEM] * 4 if resume else [IN_VMEM] * 2
    return pl.pallas_call(
        kernel,
        out_shape=RESULT if result else (STATE, STATE),
        in_specs=inputs,
        out_specs=IN_VMEM if result else (IN_VMEM, IN_VMEM),
        input_output_aliases={3: 0, 4: 1} if resume and not result else {},
        compiler_params=pltpu.CompilerParams(vmem_limit_bytes=24 * 2**20),
        cost_estimate=pl.CostEstimate(
            flops=count * single * 4 * HEAD, bytes_accessed=2**22, transcendentals=2 * count * single
        ),
    )(*args)


def body(hidden, queries, down_weight, up_weight, lengths):
    _, rows, _ = hidden.shape
    depth, rank2 = down_weight.shape
    rank = rank2 // 2
    piece, kv_width = up_weight.shape[1:]
    groups = kv_width // HEAD
    hidden = hidden[0]
    core = lax.axis_index("core")
    mine = 2 * lax.axis_index("xl") + core
    plane = lax.axis_index("z")
    start = lax.axis_index(SEQ_AXES) * rows
    info = jnp.stack([mine, plane]).astype(jnp.int32)

    share = RELAYED // 4
    split = depth - RELAYED
    forward, crossed = x_step(0), x_step(1)

    def columns(which, first, count):
        return lax.dynamic_slice(down_weight, (first, rank * which), (count, rank))

    def direct_rows(which):
        upper = lax.dynamic_index_in_dim(up_weight, which, 0, keepdims=False)
        return jnp.concatenate(
            [columns(which, 0, split), upper[:, :rank], upper[:, rank:]], axis=0
        )

    first = split + share * plane
    relay_a = lax.ppermute(columns(core, first, share), X_AXES, forward)
    relay_b = lax.ppermute(columns(1 - core, first, share), X_AXES, crossed)
    direct_a = lax.ppermute(direct_rows(core), X_AXES, forward)
    direct_b = lax.ppermute(direct_rows(1 - core), X_AXES, crossed)
    relay_own = jnp.stack([relay_a, relay_b])
    relays = [lax.ppermute(relay_own, "z", ring(k)) for k in (1, -1, 2)]
    partner_hidden = to_partner(hidden)
    partner_weight = to_partner(down_weight)
    partner_upper = to_partner(up_weight)

    half = HEAD // 2
    places = (start + jnp.arange(rows, dtype=jnp.int32)).astype(jnp.float32)
    freqs = 10000.0 ** (-2.0 * jnp.arange(half, dtype=jnp.float32) / HEAD)
    angles = places[:, None] * freqs[None, :]
    cosine, sine = jnp.cos(angles), jnp.sin(angles)
    cosine = jnp.where(core == 0, jnp.concatenate([cosine, cosine], axis=1), 1.0)
    sine = jnp.where(core == 0, jnp.concatenate([-sine, sine], axis=1), 0.0)

    def hidden_part(flip):
        return pl.BlockSpec((rows, depth), lambda i, s: (0, s[0] ^ flip))

    def whole(shape):
        return pl.BlockSpec(shape, lambda i, s: (0,) * len(shape))

    half_weight = pl.BlockSpec((depth, rank), lambda i, s: (0, s[0] % 2))
    half_upper = pl.BlockSpec((1, piece, kv_width), lambda i, s: (s[0] % 2, 0, 0))

    def projection(kernel, **spec):
        out_shape = spec.pop("out_shape")
        return pl.pallas_call(
            kernel,
            out_shape=out_shape,
            grid_spec=pltpu.PrefetchScalarGridSpec(num_scalar_prefetch=1, grid=(1,), **spec),
            compiler_params=pltpu.CompilerParams(vmem_limit_bytes=40 * 2**20),
            cost_estimate=pl.CostEstimate(
                flops=4 * rows * depth * rank2, bytes_accessed=8 * 2**20, transcendentals=0
            ),
        )

    partial = projection(
        half_product_kernel,
        out_shape=jax.ShapeDtypeStruct((2 * rows, rank), jnp.float32),
        in_specs=[hidden_part(0), hidden_part(1)] * 2 + [half_weight] * 2,
        out_specs=whole((2 * rows, rank)),
    )(info, hidden, hidden, partner_hidden, partner_hidden, down_weight, partner_weight)

    latent, pairs = projection(
        project_kernel,
        out_shape=(
            jax.ShapeDtypeStruct((2 * rows, rank), jnp.bfloat16),
            jax.ShapeDtypeStruct((2 * groups, rows, HEAD), jnp.bfloat16),
        ),
        in_specs=[whole((2 * rows, rank))]
        + [hidden_part(2), hidden_part(3)] * 2
        + [whole((split + 2 * piece, rank))] * 2
        + [whole((2, share, rank))] * 4
        + [half_upper] * 2
        + [whole((rows, HEAD))] * 2,
        out_specs=[whole((2 * rows, rank)), whole((2 * groups, rows, HEAD))],
        scratch_shapes=[
            pltpu.VMEM((2, depth, rank), jnp.bfloat16),
            pltpu.VMEM((rank, kv_width), jnp.bfloat16),
        ],
    )(
        info, partial, hidden, hidden, partner_hidden, partner_hidden, direct_a, direct_b,
        relay_own, *relays, up_weight, partner_upper, cosine, sine,
    )

    sent = queries[0].reshape(rows, groups, PAIR).transpose(1, 0, 2)
    my_queries = lax.all_to_all(sent, PLANE, 0, 0, tiled=True).reshape(CHUNK, PAIR)
    pairs, my_queries = lax.optimization_barrier((pairs, my_queries))
    own_pairs = lax.all_to_all(pairs, PLANE + ("core",), 0, 0, tiled=True)
    other_half = to_partner(latent[rows:])

    low, middle = 2 * LOW, 2 * MIDDLE
    up = [(0, 1), (1, 2), (2, 3)]
    near_low = lax.ppermute(own_pairs[:low], "z", up)
    passing = lax.ppermute(own_pairs[low:], "z", [(1, 0), (0, 3)])
    near_middle = lax.ppermute(own_pairs[low:middle], "z", up)
    near_high = lax.ppermute(own_pairs[middle:], "z", up)
    far_low = lax.ppermute(near_low, "z", [(1, 2), (2, 3)])

    spot = plane.reshape(1).astype(jnp.int32)
    state = attention_call(own_kernel, 36, (my_queries, own_pairs), resume=False)
    for name, piece_pairs in (("low", near_low), ("middle", near_middle), ("high", near_high)):
        state = attention_call(
            functools.partial(near_kernel, 2),
            piece_pairs.shape[0] // 2 * BLOCKS,
            (spot, my_queries, piece_pairs, *state),
        )
        if name == "low":
            passing, state = lax.optimization_barrier((passing, state))
            far_high = lax.ppermute(passing, "z", [(0, 3), (3, 2)])
    state = attention_call(
        functools.partial(far_kernel, LOW, False), 30,
        (spot, my_queries, far_high, *state),
    )
    result = attention_call(
        functools.partial(far_kernel, 0, True), 6,
        (spot, my_queries, far_low, *state), result=True,
    )

    home = lax.all_to_all(result.reshape(groups, rows, PAIR), PLANE, 0, 0, tiled=True)
    home = home.transpose(1, 0, 2).reshape(rows, groups * PAIR)
    live = ((start + jnp.arange(rows, dtype=jnp.int32)) < lengths[0])[:, None]
    attended = jnp.where(live, home, jnp.zeros((), jnp.bfloat16))
    ours = latent[:rows]
    both = jnp.where(
        core == 0,
        jnp.concatenate([ours, other_half], axis=1),
        jnp.concatenate([other_half, ours], axis=1),
    )
    latent = jnp.where(live, both, jnp.zeros((), jnp.bfloat16))
    return latent[None], attended[None]


def solution(mesh):
    split = Mesh(mesh.devices.reshape(tuple(SIZES.values())), tuple(SIZES))
    rows = P(DP_AXES, SEQ_AXES, None)
    placed = (rows, rows, P(DP_AXES, None), P(None, DP_AXES, None), P(DP_AXES))

    return jax.shard_map(body, mesh=split, in_specs=placed, out_specs=(rows, rows), check_vma=False)
```

```python
import functools
import itertools

import jax
import jax.numpy as jnp
from jax import lax
from jax.experimental import pallas as pl
from jax.experimental.pallas import tpu as pltpu
from jax.sharding import Mesh
from jax.sharding import PartitionSpec as P


HEAD = 128
PAIR = 2 * HEAD
BLOCK = 256
CHUNK = 2048
BLOCKS = CHUNK // BLOCK
LOW, MIDDLE = 3, 6
RELAYED = 704
SIZES = {"z": 4, "y": 4, "xh": 2, "xl": 2, "core": 2}
SEQ_AXES = ("z", "y", "xh")
DP_AXES = ("xl", "core")
PLANE = ("y", "xh")

query_scale = 144.0 ** (-0.5)
soft_cap = 50.0
LOG2E = 1.4426950408889634
CONTRACT_LAST = (((1,), (1,)), ((), ()))


X_AXES = ("xh", "xl", "core")


def x_step(flip):
    pairs = []
    for x, core in itertools.product(range(4), range(2)):
        to = (x + (1 if core == 0 else -1)) % 4
        pairs.append((2 * x + core, 2 * to + (core ^ flip)))
    return pairs


def ring(step):
    return [(i, (i + step) % 4) for i in range(4)]


def to_partner(array):
    return lax.ppermute(array, "core", [(0, 1), (1, 0)])


def pack_kernel(info, weight_a, upper_a, weight_b, upper_b, direct_a, direct_b):
    split, width = weight_a.shape
    piece = upper_a.shape[1]
    for weight, upper, direct in ((weight_a, upper_a, direct_a), (weight_b, upper_b, direct_b)):
        direct[:split, :] = weight[...]
        direct[split : split + piece, :] = upper[0, :, :width]
        direct[split + piece :, :] = upper[0, :, width:]


def both_sequences(own, partner, weight):
    stacked = jnp.concatenate([own, partner], axis=0)
    return jnp.dot(stacked, weight, preferred_element_type=jnp.float32)


def half_product_kernel(info, own_0, own_1, partner_0, partner_1, weight_0, weight_1, out):
    out[...] = both_sequences(own_0[...], partner_0[...], weight_0[...]) + both_sequences(
        own_1[...], partner_1[...], weight_1[...]
    )


def project_kernel(
    info, partial, own_2, own_3, partner_2, partner_3, direct_a, direct_b,
    relay_0, relay_1, relay_2, relay_3, up_own, up_partner, cosine, sine,
    latent, pairs, weights, upper,
):
    mine, plane = info[0], info[1]
    core = mine % 2
    rows = own_2.shape[0]
    piece = up_own.shape[1]
    share = relay_0.shape[1]
    half = direct_a.shape[1]
    split = direct_a.shape[0] - 2 * piece
    for which, direct in ((0, direct_a), (1, direct_b)):
        weights[which, :split, :] = direct[:split, :]
        for step, relay in ((0, relay_0), (3, relay_1), (1, relay_2), (2, relay_3)):
            at = split + share * ((plane + step) % 4)
            weights[which, pl.ds(pl.multiple_of(at, 16), share), :] = relay[which]
        at = pl.ds(pl.multiple_of((mine ^ (2 + which)) * piece, piece), piece)
        upper[at, :half] = direct[split : split + piece, :]
        upper[at, half:] = direct[split + piece :, :]
    upper[pl.ds(pl.multiple_of(mine * piece, piece), piece), :] = up_own[0]
    upper[pl.ds(pl.multiple_of((mine ^ 1) * piece, piece), piece), :] = up_partner[0]
    total = partial[...] + both_sequences(own_2[...], partner_2[...], weights[0])
    total = total + both_sequences(own_3[...], partner_3[...], weights[1])
    rounded = total.astype(jnp.bfloat16)
    latent[...] = rounded
    raw = jnp.dot(rounded, upper[...], preferred_element_type=jnp.float32)
    for which, turn in ((0, core), (1, 1 - core)):
        for head in range(raw.shape[1] // HEAD):
            entry = raw[which * rows : (which + 1) * rows, head * HEAD : (head + 1) * HEAD]
            entry = entry * cosine[...] + pltpu.roll(entry, HEAD // 2, 1) * sine[...]
            pairs[2 * head + turn] = entry.astype(jnp.bfloat16)


def expo(raw):
    return jnp.exp2(jnp.tanh(raw * (query_scale / soft_cap)) * (soft_cap * LOG2E))


def folded(values):
    total = values[:, :HEAD]
    for t in range(1, values.shape[1] // HEAD):
        total = total + values[:, t * HEAD : (t + 1) * HEAD]
    return total


def triangle(newer):
    row = lax.broadcasted_iota(jnp.int32, (2 * BLOCK, BLOCK), 0) % BLOCK
    col = lax.broadcasted_iota(jnp.int32, (2 * BLOCK, BLOCK), 1)
    return col <= row if newer else col > row


def stacked_rows(queries, i):
    own = queries[pl.ds(pl.multiple_of(i * BLOCK, BLOCK), BLOCK), :]
    return jnp.concatenate([own[:, :HEAD], own[:, HEAD:]], axis=0)


def over_blocks(stacked, pairs, blocks):
    numer = denom = 0.0
    for j, mask in blocks:
        raw = lax.dot_general(
            stacked, pairs[2 * j], CONTRACT_LAST, preferred_element_type=jnp.float32
        )
        e = expo(raw)
        if mask is not None:
            e = jnp.where(mask, e, 0.0)
        denom = denom + folded(e)
        numer = numer + jnp.dot(
            e.astype(jnp.bfloat16), pairs[2 * j + 1], preferred_element_type=jnp.float32
        )
    return numer, denom


def state_rows(i):
    return pl.ds(pl.multiple_of(i * 2 * BLOCK, 2 * BLOCK), 2 * BLOCK)


def own_kernel(queries, pairs, numer, denom):
    mask = triangle(True)
    for i in range(BLOCKS):
        blocks = [(j, None) for j in range(i)] + [(i, mask)]
        numer[state_rows(i), :], denom[state_rows(i), :] = over_blocks(
            stacked_rows(queries, i), pairs, blocks
        )


def near_kernel(group, info, queries, pairs, numer_in, denom_in, numer, denom):
    blocks = [(j, None) for j in range(pairs.shape[0] // 2)]

    @pl.when(info[0] >= 1)
    def _():
        def step(t, carry):
            for u in range(group):
                i = t * group + u
                n, d = over_blocks(stacked_rows(queries, i), pairs, blocks)
                numer[state_rows(i), :] += n
                denom[state_rows(i), :] += d
            return carry

        lax.fori_loop(0, BLOCKS // group, step, 0)


def far_kernel(first, last, info, queries, pairs, numer_in, denom_in, *outs):
    end = first + pairs.shape[0] // 2
    mask = triangle(False)
    numer, denom = (numer_in, denom_in) if last else outs

    def finish(i, n, d):
        if last:
            n = n / jnp.sum(d, axis=1, keepdims=True)
            outs[0][i * BLOCK : (i + 1) * BLOCK, :] = jnp.concatenate(
                [n[:BLOCK], n[BLOCK:]], axis=1
            ).astype(jnp.bfloat16)
        else:
            numer[state_rows(i), :], denom[state_rows(i), :] = n, d

    @pl.when(info[0] >= 2)
    def _():
        for i in range(BLOCKS):
            blocks = [(j - first, mask if j == i else None) for j in range(max(i, first), end)]
            old_n, old_d = numer[state_rows(i), :], denom[state_rows(i), :]
            if blocks:
                n, d = over_blocks(stacked_rows(queries, i), pairs, blocks)
                finish(i, old_n + n, old_d + d)
            elif last:
                finish(i, old_n, old_d)

    if last:

        @pl.when(info[0] < 2)
        def _():
            for i in range(BLOCKS):
                finish(i, numer[state_rows(i), :], denom[state_rows(i), :])


IN_VMEM = pl.BlockSpec(memory_space=pltpu.VMEM)
IN_SMEM = pl.BlockSpec(memory_space=pltpu.SMEM)
STATE = jax.ShapeDtypeStruct((2 * CHUNK, HEAD), jnp.float32)
RESULT = jax.ShapeDtypeStruct((CHUNK, PAIR), jnp.bfloat16)


def attention_call(kernel, count, args, result=False, resume=True):
    single = BLOCK * 2 * BLOCK
    inputs = [IN_SMEM] + [IN_VMEM] * 4 if resume else [IN_VMEM] * 2
    return pl.pallas_call(
        kernel,
        out_shape=RESULT if result else (STATE, STATE),
        in_specs=inputs,
        out_specs=IN_VMEM if result else (IN_VMEM, IN_VMEM),
        input_output_aliases={3: 0, 4: 1} if resume and not result else {},
        compiler_params=pltpu.CompilerParams(vmem_limit_bytes=12 * 2**20),
        cost_estimate=pl.CostEstimate(
            flops=count * single * 4 * HEAD, bytes_accessed=2**22, transcendentals=2 * count * single
        ),
    )(*args)


def body(hidden, queries, down_weight, up_weight, lengths):
    _, rows, _ = hidden.shape
    depth, rank2 = down_weight.shape
    rank = rank2 // 2
    piece, kv_width = up_weight.shape[1:]
    groups = kv_width // HEAD
    hidden = hidden[0]
    core = lax.axis_index("core")
    mine = 2 * lax.axis_index("xl") + core
    plane = lax.axis_index("z")
    start = lax.axis_index(SEQ_AXES) * rows
    info = jnp.stack([mine, plane]).astype(jnp.int32)

    share = RELAYED // 4
    split = depth - RELAYED
    forward, crossed = x_step(0), x_step(1)

    def columns(which, first, count):
        return lax.dynamic_slice(down_weight, (first, rank * which), (count, rank))

    first = split + share * plane
    relay_a = lax.ppermute(columns(core, first, share), X_AXES, forward)
    relay_b = lax.ppermute(columns(1 - core, first, share), X_AXES, crossed)
    packed = jax.ShapeDtypeStruct((split + 2 * piece, rank), jnp.bfloat16)

    def packing(flip):
        return [
            pl.BlockSpec((split, rank), lambda i, s: (0, (s[0] ^ flip) % 2)),
            pl.BlockSpec((1, piece, kv_width), lambda i, s: ((s[0] ^ flip) % 2, 0, 0)),
        ]

    direct_a, direct_b = pl.pallas_call(
        pack_kernel,
        out_shape=(packed, packed),
        grid_spec=pltpu.PrefetchScalarGridSpec(
            num_scalar_prefetch=1,
            grid=(1,),
            in_specs=packing(0) + packing(1),
            out_specs=[pl.BlockSpec(packed.shape, lambda i, s: (0, 0))] * 2,
        ),
        compiler_params=pltpu.CompilerParams(vmem_limit_bytes=16 * 2**20),
        cost_estimate=pl.CostEstimate(flops=10**6, bytes_accessed=2**22, transcendentals=0),
        name="pack",
    )(info, down_weight, up_weight, down_weight, up_weight)
    direct_a = lax.ppermute(direct_a, X_AXES, forward)
    direct_b = lax.ppermute(direct_b, X_AXES, crossed)
    relay_own = jnp.stack([relay_a, relay_b])
    relays = [lax.ppermute(relay_own, "z", ring(k)) for k in (1, -1, 2)]
    partner_hidden = to_partner(hidden)
    partner_weight = to_partner(down_weight)
    partner_upper = to_partner(up_weight)

    sent = queries[0].reshape(rows, 4, 2, PAIR).transpose(1, 2, 0, 3)
    sent = lax.all_to_all(sent, "y", 0, 0, tiled=True)
    here = lax.axis_index("xh")
    kept_queries = lax.dynamic_index_in_dim(sent, here, 1, keepdims=False)
    leaving = lax.dynamic_index_in_dim(sent, 1 - here, 1, keepdims=False)
    leaving, direct_a, direct_b = lax.optimization_barrier((leaving, direct_a, direct_b))
    crossing_queries = lax.ppermute(leaving, "xh", [(0, 1), (1, 0)])

    half = HEAD // 2
    places = (start + jnp.arange(rows, dtype=jnp.int32)).astype(jnp.float32)
    freqs = 10000.0 ** (-2.0 * jnp.arange(half, dtype=jnp.float32) / HEAD)
    angles = places[:, None] * freqs[None, :]
    cosine, sine = jnp.cos(angles), jnp.sin(angles)
    cosine = jnp.where(core == 0, jnp.concatenate([cosine, cosine], axis=1), 1.0)
    sine = jnp.where(core == 0, jnp.concatenate([-sine, sine], axis=1), 0.0)

    def hidden_part(flip):
        return pl.BlockSpec((rows, depth), lambda i, s: (0, s[0] ^ flip))

    def whole(shape):
        return pl.BlockSpec(shape, lambda i, s: (0,) * len(shape))

    half_weight = pl.BlockSpec((depth, rank), lambda i, s: (0, s[0] % 2))
    half_upper = pl.BlockSpec((1, piece, kv_width), lambda i, s: (s[0] % 2, 0, 0))

    def projection(kernel, **spec):
        out_shape = spec.pop("out_shape")
        return pl.pallas_call(
            kernel,
            out_shape=out_shape,
            grid_spec=pltpu.PrefetchScalarGridSpec(num_scalar_prefetch=1, grid=(1,), **spec),
            compiler_params=pltpu.CompilerParams(vmem_limit_bytes=26 * 2**20),
            cost_estimate=pl.CostEstimate(
                flops=4 * rows * depth * rank2, bytes_accessed=8 * 2**20, transcendentals=0
            ),
        )

    partial = projection(
        half_product_kernel,
        out_shape=jax.ShapeDtypeStruct((2 * rows, rank), jnp.float32),
        in_specs=[hidden_part(0), hidden_part(1)] * 2 + [half_weight] * 2,
        out_specs=whole((2 * rows, rank)),
    )(info, hidden, hidden, partner_hidden, partner_hidden, down_weight, partner_weight)

    latent, pairs = projection(
        project_kernel,
        out_shape=(
            pltpu.HBM((2 * rows, rank), jnp.bfloat16),
            pltpu.HBM((2 * groups, rows, HEAD), jnp.bfloat16),
        ),
        in_specs=[whole((2 * rows, rank))]
        + [hidden_part(2), hidden_part(3)] * 2
        + [whole((split + 2 * piece, rank))] * 2
        + [whole((2, share, rank))] * 4
        + [half_upper] * 2
        + [whole((rows, HEAD))] * 2,
        out_specs=[whole((2 * rows, rank)), whole((2 * groups, rows, HEAD))],
        scratch_shapes=[
            pltpu.VMEM((2, depth, rank), jnp.bfloat16),
            pltpu.VMEM((rank, kv_width), jnp.bfloat16),
        ],
    )(
        info, partial, hidden, hidden, partner_hidden, partner_hidden, direct_a, direct_b,
        relay_own, *relays, up_weight, partner_upper, cosine, sine,
    )

    mixed = jnp.stack([kept_queries, crossing_queries], axis=1)
    ordered = jnp.where(lax.axis_index("xh") == 0, mixed, mixed[:, ::-1])
    my_queries = ordered.reshape(CHUNK, PAIR)
    own_pairs = lax.all_to_all(pairs, PLANE + ("core",), 0, 0, tiled=True)
    other_half = to_partner(latent[rows:])

    low, middle = 2 * LOW, 2 * MIDDLE
    up = [(0, 1), (1, 2), (2, 3)]
    near_low = lax.ppermute(own_pairs[:low], "z", up)
    passing = lax.ppermute(own_pairs[low:], "z", [(1, 0), (0, 3)])
    near_middle = lax.ppermute(own_pairs[low:middle], "z", up)
    near_high = lax.ppermute(own_pairs[middle:], "z", up)
    far_low = lax.ppermute(near_low, "z", [(1, 2), (2, 3)])

    spot = plane.reshape(1).astype(jnp.int32)
    state = attention_call(own_kernel, 36, (my_queries, own_pairs), resume=False)
    passing, state = lax.optimization_barrier((passing, state))
    far_high = lax.ppermute(passing, "z", [(0, 3), (3, 2)])
    for piece_pairs in (near_low, near_middle, near_high):
        state = attention_call(
            functools.partial(near_kernel, 4),
            piece_pairs.shape[0] // 2 * BLOCKS,
            (spot, my_queries, piece_pairs, *state),
        )
    state = attention_call(
        functools.partial(far_kernel, LOW, False), 30,
        (spot, my_queries, far_high, *state),
    )
    result = attention_call(
        functools.partial(far_kernel, 0, True), 6,
        (spot, my_queries, far_low, *state), result=True,
    )

    home = lax.all_to_all(result.reshape(groups, rows, PAIR), PLANE, 0, 0, tiled=True)
    home = home.transpose(1, 0, 2).reshape(rows, groups * PAIR)
    live = ((start + jnp.arange(rows, dtype=jnp.int32)) < lengths[0])[:, None]
    attended = jnp.where(live, home, jnp.zeros((), jnp.bfloat16))
    ours = latent[:rows]
    both = jnp.where(
        core == 0,
        jnp.concatenate([ours, other_half], axis=1),
        jnp.concatenate([other_half, ours], axis=1),
    )
    latent = jnp.where(live, both, jnp.zeros((), jnp.bfloat16))
    return latent[None], attended[None]


def solution(mesh):
    split = Mesh(mesh.devices.reshape(tuple(SIZES.values())), tuple(SIZES))
    rows = P(DP_AXES, SEQ_AXES, None)
    placed = (rows, rows, P(DP_AXES, None), P(None, DP_AXES, None), P(DP_AXES))

    return jax.shard_map(body, mesh=split, in_specs=placed, out_specs=(rows, rows), check_vma=False)
```

```python
import functools
import itertools

import jax
import jax.numpy as jnp
from jax import lax
from jax.experimental import pallas as pl
from jax.experimental.pallas import tpu as pltpu
from jax.sharding import Mesh
from jax.sharding import PartitionSpec as P


HEAD = 128
PAIR = 2 * HEAD
BLOCK = 256
CHUNK = 2048
BLOCKS = CHUNK // BLOCK
LOW, MIDDLE = 4, 6
RELAYED = 576
SIZES = {"z": 4, "y": 4, "xh": 2, "xl": 2, "core": 2}
SEQ_AXES = ("z", "y", "xh")
DP_AXES = ("xl", "core")
PLANE = ("y", "xh")

query_scale = 144.0 ** (-0.5)
soft_cap = 50.0
LOG2E = 1.4426950408889634
CONTRACT_LAST = (((1,), (1,)), ((), ()))


X_AXES = ("xh", "xl", "core")


def x_step(flip):
    pairs = []
    for x, core in itertools.product(range(4), range(2)):
        to = (x + (1 if core == 0 else -1)) % 4
        pairs.append((2 * x + core, 2 * to + (core ^ flip)))
    return pairs


def ring(step):
    return [(i, (i + step) % 4) for i in range(4)]


def to_partner(array):
    return lax.ppermute(array, "core", [(0, 1), (1, 0)])


def pack_kernel(info, weight_a, upper_a, weight_b, upper_b, direct_a, direct_b):
    split, width = weight_a.shape
    piece = upper_a.shape[1]
    for weight, upper, direct in ((weight_a, upper_a, direct_a), (weight_b, upper_b, direct_b)):
        direct[:split, :] = weight[...]
        direct[split : split + piece, :] = upper[0, :, :width]
        direct[split + piece :, :] = upper[0, :, width:]


def both_sequences(own, partner, weight):
    stacked = jnp.concatenate([own, partner], axis=0)
    return jnp.dot(stacked, weight, preferred_element_type=jnp.float32)


def half_product_kernel(info, own_0, own_1, partner_0, partner_1, weight_0, weight_1, out):
    out[...] = both_sequences(own_0[...], partner_0[...], weight_0[...]) + both_sequences(
        own_1[...], partner_1[...], weight_1[...]
    )


def project_kernel(
    info, partial, own_2, own_3, partner_2, partner_3, direct_a, direct_b,
    relay_0, relay_1, relay_2, relay_3, up_own, up_partner, cosine, sine,
    latent, pairs, weights, upper,
):
    mine, plane = info[0], info[1]
    core = mine % 2
    rows = own_2.shape[0]
    piece = up_own.shape[1]
    share = relay_0.shape[1]
    half = direct_a.shape[1]
    split = direct_a.shape[0] - 2 * piece
    for which, direct in ((0, direct_a), (1, direct_b)):
        weights[which, :split, :] = direct[:split, :]
        for step, relay in ((0, relay_0), (3, relay_1), (1, relay_2), (2, relay_3)):
            at = split + share * ((plane + step) % 4)
            weights[which, pl.ds(pl.multiple_of(at, 16), share), :] = relay[which]
        at = pl.ds(pl.multiple_of((mine ^ (2 + which)) * piece, piece), piece)
        upper[at, :half] = direct[split : split + piece, :]
        upper[at, half:] = direct[split + piece :, :]
    upper[pl.ds(pl.multiple_of(mine * piece, piece), piece), :] = up_own[0]
    upper[pl.ds(pl.multiple_of((mine ^ 1) * piece, piece), piece), :] = up_partner[0]
    total = partial[...] + both_sequences(own_2[...], partner_2[...], weights[0])
    total = total + both_sequences(own_3[...], partner_3[...], weights[1])
    rounded = total.astype(jnp.bfloat16)
    latent[...] = rounded
    raw = jnp.dot(rounded, upper[...], preferred_element_type=jnp.float32)
    for which, turn in ((0, core), (1, 1 - core)):
        for head in range(raw.shape[1] // HEAD):
            entry = raw[which * rows : (which + 1) * rows, head * HEAD : (head + 1) * HEAD]
            entry = entry * cosine[...] + pltpu.roll(entry, HEAD // 2, 1) * sine[...]
            pairs[2 * head + turn] = entry.astype(jnp.bfloat16)


def expo(raw):
    return jnp.exp2(jnp.tanh(raw * (query_scale / soft_cap)) * (soft_cap * LOG2E))


def folded(values):
    total = values[:, :HEAD]
    for t in range(1, values.shape[1] // HEAD):
        total = total + values[:, t * HEAD : (t + 1) * HEAD]
    return total


def triangle(newer):
    row = lax.broadcasted_iota(jnp.int32, (2 * BLOCK, BLOCK), 0) % BLOCK
    col = lax.broadcasted_iota(jnp.int32, (2 * BLOCK, BLOCK), 1)
    return col <= row if newer else col > row


def stacked_rows(info, queries, pair, parity):
    kept, crossed = queries
    own = jnp.where(info[1] == parity, kept[pair], crossed[pair])
    return jnp.concatenate([own[:, :HEAD], own[:, HEAD:]], axis=0)


def over_blocks(stacked, pairs, blocks):
    numer = denom = 0.0
    for j, mask in blocks:
        raw = lax.dot_general(
            stacked, pairs[2 * j], CONTRACT_LAST, preferred_element_type=jnp.float32
        )
        e = expo(raw)
        if mask is not None:
            e = jnp.where(mask, e, 0.0)
        denom = denom + folded(e)
        numer = numer + jnp.dot(
            e.astype(jnp.bfloat16), pairs[2 * j + 1], preferred_element_type=jnp.float32
        )
    return numer, denom


def state_rows(i):
    return pl.ds(pl.multiple_of(i * 2 * BLOCK, 2 * BLOCK), 2 * BLOCK)


def own_kernel(info, kept, crossed, pairs, numer, denom):
    mask = triangle(True)
    for i in range(BLOCKS):
        blocks = [(j, None) for j in range(i)] + [(i, mask)]
        numer[state_rows(i), :], denom[state_rows(i), :] = over_blocks(
            stacked_rows(info, (kept, crossed), i // 2, i % 2), pairs, blocks
        )


def near_kernel(group, info, kept, crossed, pairs, numer_in, denom_in, numer, denom):
    blocks = [(j, None) for j in range(pairs.shape[0] // 2)]

    @pl.when(info[0] >= 1)
    def _():
        def step(t, carry):
            for u in range(group):
                i = t * group + u
                stacked = stacked_rows(
                    info, (kept, crossed), t * (group // 2) + u // 2, u % 2
                )
                n, d = over_blocks(stacked, pairs, blocks)
                numer[state_rows(i), :] += n
                denom[state_rows(i), :] += d
            return carry

        lax.fori_loop(0, BLOCKS // group, step, 0)


def far_kernel(first, last, info, kept, crossed, pairs, numer_in, denom_in, *outs):
    end = first + pairs.shape[0] // 2
    mask = triangle(False)
    numer, denom = (numer_in, denom_in) if last else outs

    def finish(i, n, d):
        if last:
            n = n / jnp.sum(d, axis=1, keepdims=True)
            outs[0][i * BLOCK : (i + 1) * BLOCK, :] = jnp.concatenate(
                [n[:BLOCK], n[BLOCK:]], axis=1
            ).astype(jnp.bfloat16)
        else:
            numer[state_rows(i), :], denom[state_rows(i), :] = n, d

    @pl.when(info[0] >= 2)
    def _():
        for i in range(BLOCKS):
            blocks = [(j - first, mask if j == i else None) for j in range(max(i, first), end)]
            old_n, old_d = numer[state_rows(i), :], denom[state_rows(i), :]
            if blocks:
                stacked = stacked_rows(info, (kept, crossed), i // 2, i % 2)
                n, d = over_blocks(stacked, pairs, blocks)
                finish(i, old_n + n, old_d + d)
            elif last:
                finish(i, old_n, old_d)

    if last:

        @pl.when(info[0] < 2)
        def _():
            for i in range(BLOCKS):
                finish(i, numer[state_rows(i), :], denom[state_rows(i), :])


IN_VMEM = pl.BlockSpec(memory_space=pltpu.VMEM)
IN_SMEM = pl.BlockSpec(memory_space=pltpu.SMEM)
STATE = jax.ShapeDtypeStruct((2 * CHUNK, HEAD), jnp.float32)
RESULT = jax.ShapeDtypeStruct((CHUNK, PAIR), jnp.bfloat16)


def attention_call(kernel, count, args, result=False, resume=True):
    single = BLOCK * 2 * BLOCK
    inputs = [IN_SMEM] + [IN_VMEM] * (5 if resume else 3)
    return pl.pallas_call(
        kernel,
        out_shape=RESULT if result else (STATE, STATE),
        in_specs=inputs,
        out_specs=IN_VMEM if result else (IN_VMEM, IN_VMEM),
        input_output_aliases={4: 0, 5: 1} if resume and not result else {},
        compiler_params=pltpu.CompilerParams(vmem_limit_bytes=12 * 2**20),
        cost_estimate=pl.CostEstimate(
            flops=count * single * 4 * HEAD, bytes_accessed=2**22, transcendentals=2 * count * single
        ),
    )(*args)


def body(hidden, queries, down_weight, up_weight, lengths):
    _, rows, _ = hidden.shape
    depth, rank2 = down_weight.shape
    rank = rank2 // 2
    piece, kv_width = up_weight.shape[1:]
    groups = kv_width // HEAD
    hidden = hidden[0]
    core = lax.axis_index("core")
    mine = 2 * lax.axis_index("xl") + core
    plane = lax.axis_index("z")
    start = lax.axis_index(SEQ_AXES) * rows
    info = jnp.stack([mine, plane]).astype(jnp.int32)

    share = RELAYED // 4
    split = depth - RELAYED
    forward, crossed = x_step(0), x_step(1)

    def columns(which, first, count):
        return lax.dynamic_slice(down_weight, (first, rank * which), (count, rank))

    first = split + share * plane
    relay_a = lax.ppermute(columns(core, first, share), X_AXES, forward)
    relay_b = lax.ppermute(columns(1 - core, first, share), X_AXES, crossed)
    packed = jax.ShapeDtypeStruct((split + 2 * piece, rank), jnp.bfloat16)

    def packing(flip):
        return [
            pl.BlockSpec((split, rank), lambda i, s: (0, (s[0] ^ flip) % 2)),
            pl.BlockSpec((1, piece, kv_width), lambda i, s: ((s[0] ^ flip) % 2, 0, 0)),
        ]

    direct_a, direct_b = pl.pallas_call(
        pack_kernel,
        out_shape=(packed, packed),
        grid_spec=pltpu.PrefetchScalarGridSpec(
            num_scalar_prefetch=1,
            grid=(1,),
            in_specs=packing(0) + packing(1),
            out_specs=[pl.BlockSpec(packed.shape, lambda i, s: (0, 0))] * 2,
        ),
        compiler_params=pltpu.CompilerParams(vmem_limit_bytes=16 * 2**20),
        cost_estimate=pl.CostEstimate(flops=10**6, bytes_accessed=2**22, transcendentals=0),
        name="pack",
    )(info, down_weight, up_weight, down_weight, up_weight)
    direct_a = lax.ppermute(direct_a, X_AXES, forward)
    direct_b = lax.ppermute(direct_b, X_AXES, crossed)
    relay_own = jnp.stack([relay_a, relay_b])
    relays = [lax.ppermute(relay_own, "z", ring(k)) for k in (1, -1, 2)]
    partner_hidden = to_partner(hidden)
    partner_weight = to_partner(down_weight)
    partner_upper = to_partner(up_weight)

    here = lax.axis_index("xh")
    split_queries = queries[0].reshape(rows, 4, 2, PAIR)
    kept_part = lax.dynamic_index_in_dim(split_queries, here, 2, keepdims=False)
    other_part = lax.dynamic_index_in_dim(split_queries, 1 - here, 2, keepdims=False)
    sent = jnp.stack([kept_part, other_part]).transpose(2, 0, 1, 3)
    sent = lax.all_to_all(sent, "y", 0, 0, tiled=True)
    kept, leaving = sent[:, 0], sent[:, 1]

    half = HEAD // 2
    places = (start + jnp.arange(rows, dtype=jnp.int32)).astype(jnp.float32)
    freqs = 10000.0 ** (-2.0 * jnp.arange(half, dtype=jnp.float32) / HEAD)
    angles = places[:, None] * freqs[None, :]
    cosine, sine = jnp.cos(angles), jnp.sin(angles)
    cosine = jnp.where(core == 0, jnp.concatenate([cosine, cosine], axis=1), 1.0)
    sine = jnp.where(core == 0, jnp.concatenate([-sine, sine], axis=1), 0.0)

    def hidden_part(flip):
        return pl.BlockSpec((rows, depth), lambda i, s: (0, s[0] ^ flip))

    def whole(shape):
        return pl.BlockSpec(shape, lambda i, s: (0,) * len(shape))

    half_weight = pl.BlockSpec((depth, rank), lambda i, s: (0, s[0] % 2))
    half_upper = pl.BlockSpec((1, piece, kv_width), lambda i, s: (s[0] % 2, 0, 0))

    def projection(kernel, **spec):
        out_shape = spec.pop("out_shape")
        return pl.pallas_call(
            kernel,
            out_shape=out_shape,
            grid_spec=pltpu.PrefetchScalarGridSpec(num_scalar_prefetch=1, grid=(1,), **spec),
            compiler_params=pltpu.CompilerParams(vmem_limit_bytes=26 * 2**20),
            cost_estimate=pl.CostEstimate(
                flops=4 * rows * depth * rank2, bytes_accessed=8 * 2**20, transcendentals=0
            ),
        )

    partial = projection(
        half_product_kernel,
        out_shape=pltpu.HBM((2 * rows, rank), jnp.float32),
        in_specs=[hidden_part(0), hidden_part(1)] * 2 + [half_weight] * 2,
        out_specs=whole((2 * rows, rank)),
    )(info, hidden, hidden, partner_hidden, partner_hidden, down_weight, partner_weight)

    latent, pairs = projection(
        project_kernel,
        out_shape=(
            pltpu.HBM((2 * rows, rank), jnp.bfloat16),
            pltpu.HBM((2 * groups, rows, HEAD), jnp.bfloat16),
        ),
        in_specs=[whole((2 * rows, rank))]
        + [hidden_part(2), hidden_part(3)] * 2
        + [whole((split + 2 * piece, rank))] * 2
        + [whole((2, share, rank))] * 4
        + [half_upper] * 2
        + [whole((rows, HEAD))] * 2,
        out_specs=[whole((2 * rows, rank)), whole((2 * groups, rows, HEAD))],
        scratch_shapes=[
            pltpu.VMEM((2, depth, rank), jnp.bfloat16),
            pltpu.VMEM((rank, kv_width), jnp.bfloat16),
        ],
    )(
        info, partial, hidden, hidden, partner_hidden, partner_hidden, direct_a, direct_b,
        relay_own, *relays, up_weight, partner_upper, cosine, sine,
    )

    leaving, pairs = lax.optimization_barrier((leaving, pairs))
    crossed_queries = lax.ppermute(leaving, "xh", [(0, 1), (1, 0)])
    own_pairs = lax.all_to_all(pairs, PLANE + ("core",), 0, 0, tiled=True)
    other_half = to_partner(latent[rows:])

    low, middle = 2 * LOW, 2 * MIDDLE
    up = [(0, 1), (1, 2), (2, 3)]
    near_low = lax.ppermute(own_pairs[:low], "z", up)
    passing = lax.ppermute(own_pairs[low:], "z", [(1, 0), (0, 3)])
    near_middle = lax.ppermute(own_pairs[low:middle], "z", up)
    near_high = lax.ppermute(own_pairs[middle:], "z", up)
    far_low = lax.ppermute(near_low, "z", [(1, 2), (2, 3)])

    common = (jnp.stack([plane, here]).astype(jnp.int32), kept, crossed_queries)
    state = attention_call(own_kernel, 36, (*common, own_pairs), resume=False)
    passing, state = lax.optimization_barrier((passing, state))
    far_high = lax.ppermute(passing, "z", [(0, 3), (3, 2)])
    for piece_pairs in (near_low, near_middle, near_high):
        state = attention_call(
            functools.partial(near_kernel, 4),
            piece_pairs.shape[0] // 2 * BLOCKS,
            (*common, piece_pairs, *state),
        )
    state = attention_call(
        functools.partial(far_kernel, LOW, False), 26,
        (*common, far_high, *state),
    )
    result = attention_call(
        functools.partial(far_kernel, 0, True), 10,
        (*common, far_low, *state), result=True,
    )

    home = lax.all_to_all(result.reshape(groups, rows, PAIR), PLANE, 0, 0, tiled=True)
    home = home.transpose(1, 0, 2).reshape(rows, groups * PAIR)
    live = ((start + jnp.arange(rows, dtype=jnp.int32)) < lengths[0])[:, None]
    attended = jnp.where(live, home, jnp.zeros((), jnp.bfloat16))
    ours = latent[:rows]
    both = jnp.where(
        core == 0,
        jnp.concatenate([ours, other_half], axis=1),
        jnp.concatenate([other_half, ours], axis=1),
    )
    latent = jnp.where(live, both, jnp.zeros((), jnp.bfloat16))
    return latent[None], attended[None]


def solution(mesh):
    split = Mesh(mesh.devices.reshape(tuple(SIZES.values())), tuple(SIZES))
    rows = P(DP_AXES, SEQ_AXES, None)
    placed = (rows, rows, P(DP_AXES, None), P(None, DP_AXES, None), P(DP_AXES))

    return jax.shard_map(body, mesh=split, in_specs=placed, out_specs=(rows, rows), check_vma=False)
```

```python
import functools
import itertools

import jax
import jax.numpy as jnp
from jax import lax
from jax.experimental import pallas as pl
from jax.experimental.pallas import tpu as pltpu
from jax.sharding import Mesh
from jax.sharding import PartitionSpec as P


HEAD = 128
PAIR = 2 * HEAD
BLOCK = 256
CHUNK = 2048
KV_HEADS = 8
BLOCKS = CHUNK // BLOCK
LOW = 4
GRANT = {"collect": 60, "half": 49, "project": 46}
RELAYED = 576
SIZES = {"z": 4, "y": 4, "xh": 2, "xl": 2, "core": 2}
SEQ_AXES = ("z", "y", "xh")
DP_AXES = ("xl", "core")
PLANE = ("y", "xh")

query_scale = 144.0 ** (-0.5)
soft_cap = 50.0
LOG2E = 1.4426950408889634
CONTRACT_LAST = (((1,), (1,)), ((), ()))


X_AXES = ("xh", "xl", "core")


def x_step(flip):
    pairs = []
    for x, core in itertools.product(range(4), range(2)):
        to = (x + (1 if core == 0 else -1)) % 4
        pairs.append((2 * x + core, 2 * to + (core ^ flip)))
    return pairs


def ring(step):
    return [(i, (i + step) % 4) for i in range(4)]


def to_partner(array):
    return lax.ppermute(array, "core", [(0, 1), (1, 0)])


def begin(sems, *moves):
    copies = [pltpu.make_async_copy(a, b, sems.at[k]) for k, (a, b) in enumerate(moves)]
    for copy in copies:
        copy.start()
    return copies


def finish(copies):
    for copy in copies:
        copy.wait()


def chunk(index, size):
    return pl.ds(pl.multiple_of(index * size, size), size)


def collect_kernel(info, down, up, queries, relay_a, relay_b, direct_a, direct_b, sent, sems):
    share, rank = relay_a.shape
    piece = up.shape[1]
    split = down.shape[0] - 4 * share
    first = pl.ds(pl.multiple_of(split + share * info[1], 16), share)
    moves = []
    for flip, relay, direct in ((0, relay_a, direct_a), (1, relay_b, direct_b)):
        which = (info[0] ^ flip) % 2
        columns = chunk(which, rank)
        moves.append((down.at[first, columns], relay))
        moves.append((down.at[pl.ds(0, split), columns], direct.at[pl.ds(0, split)]))
        for k in range(2):
            at = pl.ds(split + k * piece, piece)
            moves.append((up.at[which, :, pl.ds(k * rank, rank)], direct.at[at]))
    for y, k in itertools.product(range(4), range(2)):
        pair = 2 * y + (info[2] ^ k)
        moves.append((queries.at[:, chunk(pair, PAIR)], sent.at[y, k]))
    finish(begin(sems, *moves))


def couple_kernel(a, b, out):
    out[0] = a[...]
    out[1] = b[...]


def hidden_moves(hidden, partner, shard, into):
    rows = hidden.shape[0]
    columns = chunk(shard, into.shape[1])
    return [
        (hidden.at[:, columns], into.at[pl.ds(0, rows)]),
        (partner.at[:, columns], into.at[pl.ds(rows, rows)]),
    ]


def half_kernel(info, hidden, partner, weight_0, weight_1, out, inputs, weights, sems):
    columns = chunk(info[0] % 2, weights.shape[2])
    moves = []
    for k, weight in enumerate((weight_0, weight_1)):
        moves += hidden_moves(hidden, partner, info[0] ^ k, inputs.at[k])
        moves.append((weight.at[:, columns], weights.at[k]))
    copies = begin(sems, *moves)
    finish(copies[:3])
    total = jnp.dot(inputs[0], weights[0], preferred_element_type=jnp.float32)
    finish(copies[3:])
    out[...] = total + jnp.dot(inputs[1], weights[1], preferred_element_type=jnp.float32)


def project_kernel(
    info, partial, hidden, partner, direct_a, direct_b, relay_0, relay_1, relay_2, relay_3,
    up_own, up_partner, cosine, sine, latent, pairs,
    inputs, weights, upper, rounded, ready, sems, out_sems,
):
    mine, plane = info[0], info[1]
    core = mine % 2
    rows = hidden.shape[0]
    piece = up_own.shape[1]
    share, rank = relay_0.shape[1:]
    split = weights.shape[1] - 4 * share
    moves = []
    for which, direct in ((0, direct_a), (1, direct_b)):
        moves += hidden_moves(hidden, partner, mine ^ (2 + which), inputs.at[which])
        moves.append((direct.at[pl.ds(0, split)], weights.at[which, pl.ds(0, split)]))
        for step, relay in ((0, relay_0), (3, relay_1), (1, relay_2), (2, relay_3)):
            at = pl.multiple_of(split + share * ((plane + step) % 4), 16)
            moves.append((relay.at[which], weights.at[which, pl.ds(at, share)]))
    count = len(moves) // 2
    moves.append((up_own.at[core], upper.at[chunk(mine, piece)]))
    moves.append((up_partner.at[core], upper.at[chunk(mine ^ 1, piece)]))
    for which, direct in ((0, direct_a), (1, direct_b)):
        for k in range(2):
            at = (chunk(mine ^ (2 + which), piece), pl.ds(k * rank, rank))
            moves.append((direct.at[pl.ds(split + k * piece, piece)], upper.at[at]))
    copies = begin(sems, *moves)
    finish(copies[:count])
    total = partial[...] + jnp.dot(inputs[0], weights[0], preferred_element_type=jnp.float32)
    finish(copies[count : 2 * count])
    total = total + jnp.dot(inputs[1], weights[1], preferred_element_type=jnp.float32)
    rounded[...] = total.astype(jnp.bfloat16)
    outgoing = [pltpu.make_async_copy(rounded, latent, out_sems.at[2 * KV_HEADS])]
    outgoing[0].start()
    finish(copies[2 * count :])
    for head in range(KV_HEADS):
        raw = jnp.dot(
            rounded[...], upper[:, head * HEAD : (head + 1) * HEAD],
            preferred_element_type=jnp.float32,
        )
        for which, turn in ((0, core), (1, 1 - core)):
            entry = raw[which * rows : (which + 1) * rows]
            entry = entry * cosine[...] + pltpu.roll(entry, HEAD // 2, 1) * sine[...]
            ready[2 * head + which] = entry.astype(jnp.bfloat16)
            copy = pltpu.make_async_copy(
                ready.at[2 * head + which],
                pairs.at[2 * head + turn],
                out_sems.at[2 * head + which],
            )
            copy.start()
            outgoing.append(copy)
    finish(outgoing)


def assemble_kernel(info, home, out):
    rows = out.shape[0]
    live = (info[3] + lax.broadcasted_iota(jnp.int32, (rows, PAIR), 0)) < info[4]
    for k in range(home.shape[0]):
        part = home[k]
        out[:, k * PAIR : (k + 1) * PAIR] = jnp.where(live, part, jnp.zeros_like(part))


def expo(raw):
    return jnp.exp2(jnp.tanh(raw * (query_scale / soft_cap)) * (soft_cap * LOG2E))


def folded(values):
    total = values[:, :HEAD]
    for t in range(1, values.shape[1] // HEAD):
        total = total + values[:, t * HEAD : (t + 1) * HEAD]
    return total


def triangle(newer):
    row = lax.broadcasted_iota(jnp.int32, (2 * BLOCK, BLOCK), 0) % BLOCK
    col = lax.broadcasted_iota(jnp.int32, (2 * BLOCK, BLOCK), 1)
    return col <= row if newer else col > row


def stacked_rows(info, queries, pair, parity):
    kept, crossed = queries
    own = jnp.where(info[2] == parity, kept[pair, 0], crossed[pair])
    return jnp.concatenate([own[:, :HEAD], own[:, HEAD:]], axis=0)


def over_blocks(stacked, pairs, blocks):
    numer = denom = 0.0
    for j, mask in blocks:
        raw = lax.dot_general(
            stacked, pairs[2 * j], CONTRACT_LAST, preferred_element_type=jnp.float32
        )
        e = expo(raw)
        if mask is not None:
            e = jnp.where(mask, e, 0.0)
        denom = denom + folded(e)
        numer = numer + jnp.dot(
            e.astype(jnp.bfloat16), pairs[2 * j + 1], preferred_element_type=jnp.float32
        )
    return numer, denom


def state_rows(i):
    return pl.ds(pl.multiple_of(i * 2 * BLOCK, 2 * BLOCK), 2 * BLOCK)


def own_kernel(info, kept, crossed, pairs, numer, denom):
    mask = triangle(True)
    for i in range(BLOCKS):
        blocks = [(j, None) for j in range(i)] + [(i, mask)]
        numer[state_rows(i), :], denom[state_rows(i), :] = over_blocks(
            stacked_rows(info, (kept, crossed), i // 2, i % 2), pairs, blocks
        )


def near_kernel(group, info, kept, crossed, pairs, numer_in, denom_in, numer, denom):
    blocks = [(j, None) for j in range(pairs.shape[0] // 2)]

    @pl.when(info[1] >= 1)
    def _():
        def step(t, carry):
            for u in range(group):
                i = t * group + u
                stacked = stacked_rows(
                    info, (kept, crossed), t * (group // 2) + u // 2, u % 2
                )
                n, d = over_blocks(stacked, pairs, blocks)
                numer[state_rows(i), :] += n
                denom[state_rows(i), :] += d
            return carry

        lax.fori_loop(0, BLOCKS // group, step, 0)


def far_kernel(first, last, info, kept, crossed, pairs, numer_in, denom_in, *outs):
    end = first + pairs.shape[0] // 2
    mask = triangle(False)
    numer, denom = (numer_in, denom_in) if last else outs

    def settle(i, n, d):
        if last:
            n = n / jnp.sum(d, axis=1, keepdims=True)
            outs[0][i * BLOCK : (i + 1) * BLOCK, :] = jnp.concatenate(
                [n[:BLOCK], n[BLOCK:]], axis=1
            ).astype(jnp.bfloat16)
        else:
            numer[state_rows(i), :], denom[state_rows(i), :] = n, d

    @pl.when(info[1] >= 2)
    def _():
        for i in range(BLOCKS):
            blocks = [(j - first, mask if j == i else None) for j in range(max(i, first), end)]
            old_n, old_d = numer[state_rows(i), :], denom[state_rows(i), :]
            if blocks:
                stacked = stacked_rows(info, (kept, crossed), i // 2, i % 2)
                n, d = over_blocks(stacked, pairs, blocks)
                settle(i, old_n + n, old_d + d)
            elif last:
                settle(i, old_n, old_d)

    if last:

        @pl.when(info[1] < 2)
        def _():
            for i in range(BLOCKS):
                settle(i, numer[state_rows(i), :], denom[state_rows(i), :])


IN_VMEM = pl.BlockSpec(memory_space=pltpu.VMEM)
IN_SMEM = pl.BlockSpec(memory_space=pltpu.SMEM)
ANYWHERE = pl.BlockSpec(memory_space=pl.ANY)
STATE = jax.ShapeDtypeStruct((2 * CHUNK, HEAD), jnp.float32)
RESULT = jax.ShapeDtypeStruct((CHUNK, PAIR), jnp.bfloat16)


def attention_call(kernel, count, args, result=False, resume=True):
    single = BLOCK * 2 * BLOCK
    inputs = [IN_SMEM] + [IN_VMEM] * (5 if resume else 3)
    return pl.pallas_call(
        kernel,
        out_shape=RESULT if result else (STATE, STATE),
        in_specs=inputs,
        out_specs=IN_VMEM if result else (IN_VMEM, IN_VMEM),
        input_output_aliases={4: 0, 5: 1} if resume and not result else {},
        compiler_params=pltpu.CompilerParams(vmem_limit_bytes=12 * 2**20),
        cost_estimate=pl.CostEstimate(
            flops=count * single * 4 * HEAD, bytes_accessed=2**22, transcendentals=2 * count * single
        ),
    )(*args)


def body(hidden, queries, down_weight, up_weight, lengths):
    _, rows, _ = hidden.shape
    depth, rank2 = down_weight.shape
    rank = rank2 // 2
    piece, kv_width = up_weight.shape[1:]
    groups = kv_width // HEAD
    hidden = hidden[0]
    core = lax.axis_index("core")
    mine = 2 * lax.axis_index("xl") + core
    plane = lax.axis_index("z")
    start = lax.axis_index(SEQ_AXES) * rows
    here = lax.axis_index("xh")
    info = jnp.stack([mine, plane, here, start, lengths[0]]).astype(jnp.int32)

    share = RELAYED // 4
    split = depth - RELAYED
    forward, crossed = x_step(0), x_step(1)

    def shape(*sizes):
        return jax.ShapeDtypeStruct(sizes, jnp.bfloat16)

    def scratch(*sizes):
        return pltpu.VMEM(sizes, jnp.bfloat16)

    def step(name, kernel, out_shape, in_specs, out_specs, scratch_shapes, flops):
        return pl.pallas_call(
            kernel,
            out_shape=out_shape,
            in_specs=in_specs,
            out_specs=out_specs,
            scratch_shapes=scratch_shapes,
            compiler_params=pltpu.CompilerParams(vmem_limit_bytes=GRANT.get(name, 20) * 2**20),
            cost_estimate=pl.CostEstimate(
                flops=flops, bytes_accessed=2**22, transcendentals=0
            ),
        )

    sems = pltpu.SemaphoreType.DMA
    relay_a, relay_b, direct_a, direct_b, sent = step(
        "collect",
        collect_kernel,
        (shape(share, rank),) * 2 + (shape(split + 2 * piece, rank),) * 2
        + (shape(4, 2, rows, PAIR),),
        [IN_SMEM] + [ANYWHERE] * 3,
        (IN_VMEM,) * 5,
        [sems((16,))],
        10**8,
    )(info, down_weight, up_weight, queries[0])
    relay_a = lax.ppermute(relay_a, X_AXES, forward)
    relay_b = lax.ppermute(relay_b, X_AXES, crossed)
    direct_a = lax.ppermute(direct_a, X_AXES, forward)
    direct_b = lax.ppermute(direct_b, X_AXES, crossed)
    relay_own = step(
        "couple", couple_kernel, shape(2, share, rank), [IN_VMEM] * 2, IN_VMEM, [], 10**7
    )(relay_a, relay_b)
    relays = [lax.ppermute(relay_own, "z", ring(k)) for k in (1, -1, 2)]
    partner_hidden = to_partner(hidden)
    partner_weight = to_partner(down_weight)
    partner_upper = to_partner(up_weight)
    sent = lax.all_to_all(sent, "y", 0, 0, tiled=True)
    leaving = sent[:, 1]

    half = HEAD // 2
    places = (start + jnp.arange(rows, dtype=jnp.int32)).astype(jnp.float32)
    freqs = 10000.0 ** (-2.0 * jnp.arange(half, dtype=jnp.float32) / HEAD)
    angles = places[:, None] * freqs[None, :]
    cosine, sine = jnp.cos(angles), jnp.sin(angles)
    cosine = jnp.where(core == 0, jnp.concatenate([cosine, cosine], axis=1), 1.0)
    sine = jnp.where(core == 0, jnp.concatenate([-sine, sine], axis=1), 0.0)

    flops = 4 * rows * depth * rank2
    partial = step(
        "half",
        half_kernel,
        jax.ShapeDtypeStruct((2 * rows, rank), jnp.float32),
        [IN_SMEM] + [ANYWHERE] * 4,
        IN_VMEM,
        [scratch(2, 2 * rows, depth), scratch(2, depth, rank), sems((6,))],
        flops,
    )(info, hidden, partner_hidden, down_weight, partner_weight)

    latent, pairs = step(
        "project",
        project_kernel,
        (
            pltpu.HBM((2 * rows, rank), jnp.bfloat16),
            pltpu.HBM((2 * groups, rows, HEAD), jnp.bfloat16),
        ),
        [IN_SMEM, IN_VMEM] + [ANYWHERE] * 10 + [IN_VMEM] * 2,
        (ANYWHERE, ANYWHERE),
        [
            scratch(2, 2 * rows, depth),
            scratch(2, depth, rank),
            scratch(rank, kv_width),
            scratch(2 * rows, rank),
            scratch(2 * groups, rows, HEAD),
            sems((20,)),
            sems((2 * groups + 1,)),
        ],
        flops,
    )(
        info, partial, hidden, partner_hidden, direct_a, direct_b,
        relay_own, *relays, up_weight, partner_upper, cosine, sine,
    )

    leaving, pairs = lax.optimization_barrier((leaving, pairs))
    crossed_queries = lax.ppermute(leaving, "xh", [(0, 1), (1, 0)])
    own_pairs = lax.all_to_all(pairs, PLANE + ("core",), 0, 0, tiled=True)
    other_half = to_partner(latent[rows:])

    low = 2 * LOW
    up = [(0, 1), (1, 2), (2, 3)]
    near_low = lax.ppermute(own_pairs[:low], "z", up)
    passing = lax.ppermute(own_pairs[low:], "z", [(1, 0), (0, 3)])
    near_high = lax.ppermute(own_pairs[low:], "z", up)
    far_low = lax.ppermute(near_low, "z", [(1, 2), (2, 3)])

    common = (info, sent, crossed_queries)
    state = attention_call(own_kernel, 36, (*common, own_pairs), resume=False)
    passing, state = lax.optimization_barrier((passing, state))
    far_high = lax.ppermute(passing, "z", [(0, 3), (3, 2)])
    for piece_pairs in (near_low, near_high):
        state = attention_call(
            functools.partial(near_kernel, 4),
            piece_pairs.shape[0] // 2 * BLOCKS,
            (*common, piece_pairs, *state),
        )
    state = attention_call(
        functools.partial(far_kernel, LOW, False), 26,
        (*common, far_high, *state),
    )
    result = attention_call(
        functools.partial(far_kernel, 0, True), 10,
        (*common, far_low, *state), result=True,
    )

    home = lax.all_to_all(result.reshape(groups, rows, PAIR), PLANE, 0, 0, tiled=True)
    each = 2
    attended = pl.pallas_call(
        assemble_kernel,
        out_shape=shape(rows, groups * PAIR),
        grid_spec=pltpu.PrefetchScalarGridSpec(
            num_scalar_prefetch=1,
            grid=(groups // each,),
            in_specs=[pl.BlockSpec((each, rows, PAIR), lambda i, s: (i, 0, 0))],
            out_specs=pl.BlockSpec((rows, each * PAIR), lambda i, s: (0, i)),
        ),
        compiler_params=pltpu.CompilerParams(vmem_limit_bytes=8 * 2**20),
        name="assemble",
    )(info, home)
    live = ((start + jnp.arange(rows, dtype=jnp.int32)) < lengths[0])[:, None]
    ours = latent[:rows]
    both = jnp.where(
        core == 0,
        jnp.concatenate([ours, other_half], axis=1),
        jnp.concatenate([other_half, ours], axis=1),
    )
    latent = jnp.where(live, both, jnp.zeros((), jnp.bfloat16))
    return latent[None], attended[None]


def solution(mesh):
    split = Mesh(mesh.devices.reshape(tuple(SIZES.values())), tuple(SIZES))
    rows = P(DP_AXES, SEQ_AXES, None)
    placed = (rows, rows, P(DP_AXES, None), P(None, DP_AXES, None), P(DP_AXES))

    return jax.shard_map(body, mesh=split, in_specs=placed, out_specs=(rows, rows), check_vma=False)
```

```python
import functools
import itertools

import jax
import jax.numpy as jnp
from jax import lax
from jax.experimental import pallas as pl
from jax.experimental.pallas import tpu as pltpu
from jax.sharding import Mesh
from jax.sharding import PartitionSpec as P


HEAD = 128
PAIR = 2 * HEAD
BLOCK = 256
CHUNK = 2048
KV_HEADS = 8
BLOCKS = CHUNK // BLOCK
LOW, TOP, MIDDLE = 3, 5, 6
GRANT = {"first": 60, "collect": 60, "half": 49, "project": 46}
RELAYED = 576
SIZES = {"z": 4, "y": 4, "xh": 2, "xl": 2, "core": 2}
SEQ_AXES = ("z", "y", "xh")
DP_AXES = ("xl", "core")
PLANE = ("y", "xh")

query_scale = 144.0 ** (-0.5)
soft_cap = 50.0
LOG2E = 1.4426950408889634
CONTRACT_LAST = (((1,), (1,)), ((), ()))


X_AXES = ("xh", "xl", "core")


def x_step(flip):
    pairs = []
    for x, core in itertools.product(range(4), range(2)):
        to = (x + (1 if core == 0 else -1)) % 4
        pairs.append((2 * x + core, 2 * to + (core ^ flip)))
    return pairs


def ring(step):
    return [(i, (i + step) % 4) for i in range(4)]


def to_partner(array):
    return lax.ppermute(array, "core", [(0, 1), (1, 0)])


def begin(sems, *moves):
    copies = [pltpu.make_async_copy(a, b, sems.at[k]) for k, (a, b) in enumerate(moves)]
    for copy in copies:
        copy.start()
    return copies


def finish(copies):
    for copy in copies:
        copy.wait()


def chunk(index, size):
    return pl.ds(pl.multiple_of(index * size, size), size)


def first_kernel(info, down, relay_a, relay_b, sems):
    share, rank = relay_a.shape
    split = down.shape[0] - 4 * share
    rows = pl.ds(pl.multiple_of(split + share * info[1], 16), share)
    moves = []
    for flip, relay in ((0, relay_a), (1, relay_b)):
        moves.append((down.at[rows, chunk((info[0] ^ flip) % 2, rank)], relay))
    finish(begin(sems, *moves))


def collect_kernel(info, down, up, queries, direct_a, direct_b, sent, sems):
    rank = direct_a.shape[1]
    piece = up.shape[1]
    split = direct_a.shape[0] - 2 * piece
    moves = []
    for flip, direct in ((0, direct_a), (1, direct_b)):
        which = (info[0] ^ flip) % 2
        columns = chunk(which, rank)
        moves.append((down.at[pl.ds(0, split), columns], direct.at[pl.ds(0, split)]))
        for k in range(2):
            at = pl.ds(split + k * piece, piece)
            moves.append((up.at[which, :, pl.ds(k * rank, rank)], direct.at[at]))
    for y, k in itertools.product(range(4), range(2)):
        pair = 2 * y + (info[2] ^ k)
        moves.append((queries.at[:, chunk(pair, PAIR)], sent.at[y, k]))
    finish(begin(sems, *moves))


def couple_kernel(a, b, out):
    out[0] = a[...]
    out[1] = b[...]


def hidden_moves(hidden, partner, shard, into):
    rows = hidden.shape[0]
    columns = chunk(shard, into.shape[1])
    return [
        (hidden.at[:, columns], into.at[pl.ds(0, rows)]),
        (partner.at[:, columns], into.at[pl.ds(rows, rows)]),
    ]


def half_kernel(info, hidden, partner, weight_0, weight_1, out, inputs, weights, sems):
    columns = chunk(info[0] % 2, weights.shape[2])
    moves = []
    for k, weight in enumerate((weight_0, weight_1)):
        moves += hidden_moves(hidden, partner, info[0] ^ k, inputs.at[k])
        moves.append((weight.at[:, columns], weights.at[k]))
    copies = begin(sems, *moves)
    finish(copies[:3])
    total = jnp.dot(inputs[0], weights[0], preferred_element_type=jnp.float32)
    finish(copies[3:])
    out[...] = total + jnp.dot(inputs[1], weights[1], preferred_element_type=jnp.float32)


def project_kernel(
    info, partial, hidden, partner, direct_a, direct_b, relay_0, relay_1, relay_2, relay_3,
    up_own, up_partner, cosine, sine, latent, pairs,
    inputs, weights, upper, rounded, ready, sems, out_sems,
):
    mine, plane = info[0], info[1]
    core = mine % 2
    rows = hidden.shape[0]
    piece = up_own.shape[1]
    share, rank = relay_0.shape[1:]
    split = weights.shape[1] - 4 * share
    moves = []
    for which, direct in ((0, direct_a), (1, direct_b)):
        moves += hidden_moves(hidden, partner, mine ^ (2 + which), inputs.at[which])
        moves.append((direct.at[pl.ds(0, split)], weights.at[which, pl.ds(0, split)]))
        for step, relay in ((0, relay_0), (3, relay_1), (1, relay_2), (2, relay_3)):
            at = pl.multiple_of(split + share * ((plane + step) % 4), 16)
            moves.append((relay.at[which], weights.at[which, pl.ds(at, share)]))
    count = len(moves) // 2
    moves.append((up_own.at[core], upper.at[chunk(mine, piece)]))
    moves.append((up_partner.at[core], upper.at[chunk(mine ^ 1, piece)]))
    for which, direct in ((0, direct_a), (1, direct_b)):
        for k in range(2):
            at = (chunk(mine ^ (2 + which), piece), pl.ds(k * rank, rank))
            moves.append((direct.at[pl.ds(split + k * piece, piece)], upper.at[at]))
    copies = begin(sems, *moves)
    finish(copies[:count])
    total = partial[...] + jnp.dot(inputs[0], weights[0], preferred_element_type=jnp.float32)
    finish(copies[count : 2 * count])
    total = total + jnp.dot(inputs[1], weights[1], preferred_element_type=jnp.float32)
    rounded[...] = total.astype(jnp.bfloat16)
    outgoing = [pltpu.make_async_copy(rounded, latent, out_sems.at[2 * KV_HEADS])]
    outgoing[0].start()
    finish(copies[2 * count :])
    for head in range(KV_HEADS):
        raw = jnp.dot(
            rounded[...], upper[:, head * HEAD : (head + 1) * HEAD],
            preferred_element_type=jnp.float32,
        )
        for which, turn in ((0, core), (1, 1 - core)):
            entry = raw[which * rows : (which + 1) * rows]
            entry = entry * cosine[...] + pltpu.roll(entry, HEAD // 2, 1) * sine[...]
            ready[2 * head + which] = entry.astype(jnp.bfloat16)
            copy = pltpu.make_async_copy(
                ready.at[2 * head + which],
                pairs.at[2 * head + turn],
                out_sems.at[2 * head + which],
            )
            copy.start()
            outgoing.append(copy)
    finish(outgoing)


def assemble_kernel(info, home, out):
    rows = out.shape[0]
    live = (info[3] + lax.broadcasted_iota(jnp.int32, (rows, PAIR), 0)) < info[4]
    for k in range(home.shape[0]):
        part = home[k]
        out[:, k * PAIR : (k + 1) * PAIR] = jnp.where(live, part, jnp.zeros_like(part))


def expo(raw):
    return jnp.exp2(jnp.tanh(raw * (query_scale / soft_cap)) * (soft_cap * LOG2E))


def folded(values):
    total = values[:, :HEAD]
    for t in range(1, values.shape[1] // HEAD):
        total = total + values[:, t * HEAD : (t + 1) * HEAD]
    return total


def triangle(newer):
    row = lax.broadcasted_iota(jnp.int32, (2 * BLOCK, BLOCK), 0) % BLOCK
    col = lax.broadcasted_iota(jnp.int32, (2 * BLOCK, BLOCK), 1)
    return col <= row if newer else col > row


def stacked_rows(info, queries, pair, parity):
    kept, crossed = queries
    own = jnp.where(info[2] == parity, kept[pair, 0], crossed[pair])
    return jnp.concatenate([own[:, :HEAD], own[:, HEAD:]], axis=0)


def over_blocks(stacked, pairs, blocks):
    numer = denom = 0.0
    for j, mask in blocks:
        raw = lax.dot_general(
            stacked, pairs[2 * j], CONTRACT_LAST, preferred_element_type=jnp.float32
        )
        e = expo(raw)
        if mask is not None:
            e = jnp.where(mask, e, 0.0)
        denom = denom + folded(e)
        numer = numer + jnp.dot(
            e.astype(jnp.bfloat16), pairs[2 * j + 1], preferred_element_type=jnp.float32
        )
    return numer, denom


def state_rows(i):
    return pl.ds(pl.multiple_of(i * 2 * BLOCK, 2 * BLOCK), 2 * BLOCK)


def own_kernel(info, kept, crossed, pairs, numer, denom):
    mask = triangle(True)
    for i in range(BLOCKS):
        blocks = [(j, None) for j in range(i)] + [(i, mask)]
        numer[state_rows(i), :], denom[state_rows(i), :] = over_blocks(
            stacked_rows(info, (kept, crossed), i // 2, i % 2), pairs, blocks
        )


def two_blocks(info, queries, pair):
    return jnp.concatenate(
        [stacked_rows(info, queries, pair, 0), stacked_rows(info, queries, pair, 1)], axis=0
    )


def pair_rows(pair):
    return chunk(pair, 4 * BLOCK)


def near_kernel(info, kept, crossed, pairs, numer_in, denom_in, numer, denom):
    blocks = [(j, None) for j in range(pairs.shape[0] // 2)]

    @pl.when(info[1] >= 1)
    def _():
        def step(t, carry):
            for u in range(2):
                pair = 2 * t + u
                n, d = over_blocks(two_blocks(info, (kept, crossed), pair), pairs, blocks)
                numer[pair_rows(pair), :] += n
                denom[pair_rows(pair), :] += d
            return carry

        lax.fori_loop(0, BLOCKS // 4, step, 0)


def far_kernel(pieces, last, info, kept, crossed, *refs):
    inputs, refs = refs[: len(pieces)], refs[len(pieces) :]
    if last:
        numer, denom, out = refs
    else:
        _, _, numer, denom = refs
    single = triangle(False)
    row = lax.broadcasted_iota(jnp.int32, (4 * BLOCK, BLOCK), 0)
    col = lax.broadcasted_iota(jnp.int32, (4 * BLOCK, BLOCK), 1)
    double = (row < 2 * BLOCK) | (col > row % BLOCK)

    def settle(pair, n, d):
        at = pair_rows(pair)
        if not last:
            numer[at, :], denom[at, :] = n, d
            return
        result = n / jnp.sum(d, axis=1, keepdims=True)
        for k in range(2):
            own = result[2 * k * BLOCK : 2 * (k + 1) * BLOCK]
            out[chunk(2 * pair + k, BLOCK), :] = jnp.concatenate(
                [own[:BLOCK], own[BLOCK:]], axis=1
            ).astype(jnp.bfloat16)

    @pl.when(info[1] >= 2)
    def _():
        for pair in range(BLOCKS // 2):
            i = 2 * pair
            n, d = numer[pair_rows(pair), :], denom[pair_rows(pair), :]
            touched = False
            for ref, (first, end) in zip(inputs, pieces):
                shared = [
                    (j - first, double if j == i + 1 else None)
                    for j in range(max(i + 1, first), end)
                ]
                if shared:
                    more = over_blocks(two_blocks(info, (kept, crossed), pair), ref, shared)
                    n, d, touched = n + more[0], d + more[1], True
                if first <= i < end:
                    own = stacked_rows(info, (kept, crossed), pair, 0)
                    more = over_blocks(own, ref, [(i - first, single)])
                    rest = jnp.zeros((2 * BLOCK, HEAD), jnp.float32)
                    n = n + jnp.concatenate([more[0], rest], axis=0)
                    d = d + jnp.concatenate([more[1], rest], axis=0)
                    touched = True
            if touched or last:
                settle(pair, n, d)

    if last:

        @pl.when(info[1] < 2)
        def _():
            for pair in range(BLOCKS // 2):
                settle(pair, numer[pair_rows(pair), :], denom[pair_rows(pair), :])


IN_VMEM = pl.BlockSpec(memory_space=pltpu.VMEM)
IN_SMEM = pl.BlockSpec(memory_space=pltpu.SMEM)
ANYWHERE = pl.BlockSpec(memory_space=pl.ANY)
STATE = jax.ShapeDtypeStruct((2 * CHUNK, HEAD), jnp.float32)
RESULT = jax.ShapeDtypeStruct((CHUNK, PAIR), jnp.bfloat16)


def attention_call(kernel, count, args, result=False, resume=True):
    single = BLOCK * 2 * BLOCK
    state = len(args) - 2
    return pl.pallas_call(
        kernel,
        out_shape=RESULT if result else (STATE, STATE),
        in_specs=[IN_SMEM] + [IN_VMEM] * (len(args) - 1),
        out_specs=IN_VMEM if result else (IN_VMEM, IN_VMEM),
        input_output_aliases={state: 0, state + 1: 1} if resume and not result else {},
        compiler_params=pltpu.CompilerParams(vmem_limit_bytes=12 * 2**20),
        cost_estimate=pl.CostEstimate(
            flops=count * single * 4 * HEAD, bytes_accessed=2**22, transcendentals=2 * count * single
        ),
    )(*args)


def body(hidden, queries, down_weight, up_weight, lengths):
    _, rows, _ = hidden.shape
    depth, rank2 = down_weight.shape
    rank = rank2 // 2
    piece, kv_width = up_weight.shape[1:]
    groups = kv_width // HEAD
    hidden = hidden[0]
    core = lax.axis_index("core")
    mine = 2 * lax.axis_index("xl") + core
    plane = lax.axis_index("z")
    start = lax.axis_index(SEQ_AXES) * rows
    here = lax.axis_index("xh")
    info = jnp.stack([mine, plane, here, start, lengths[0]]).astype(jnp.int32)

    share = RELAYED // 4
    split = depth - RELAYED
    forward, crossed = x_step(0), x_step(1)

    def shape(*sizes):
        return jax.ShapeDtypeStruct(sizes, jnp.bfloat16)

    def scratch(*sizes):
        return pltpu.VMEM(sizes, jnp.bfloat16)

    def step(name, kernel, out_shape, in_specs, out_specs, scratch_shapes, flops):
        return pl.pallas_call(
            kernel,
            out_shape=out_shape,
            in_specs=in_specs,
            out_specs=out_specs,
            scratch_shapes=scratch_shapes,
            compiler_params=pltpu.CompilerParams(vmem_limit_bytes=GRANT.get(name, 20) * 2**20),
            cost_estimate=pl.CostEstimate(
                flops=flops, bytes_accessed=2**22, transcendentals=0
            ),
        )

    sems = pltpu.SemaphoreType.DMA
    relay_a, relay_b = step(
        "first",
        first_kernel,
        (shape(share, rank),) * 2,
        [IN_SMEM, ANYWHERE],
        (IN_VMEM,) * 2,
        [sems((2,))],
        10**7,
    )(info, down_weight)
    direct_a, direct_b, sent = step(
        "collect",
        collect_kernel,
        (shape(split + 2 * piece, rank),) * 2 + (shape(4, 2, rows, PAIR),),
        [IN_SMEM] + [ANYWHERE] * 3,
        (IN_VMEM,) * 3,
        [sems((14,))],
        10**8,
    )(info, down_weight, up_weight, queries[0])
    relay_a = lax.ppermute(relay_a, X_AXES, forward)
    relay_b = lax.ppermute(relay_b, X_AXES, crossed)
    direct_a = lax.ppermute(direct_a, X_AXES, forward)
    direct_b = lax.ppermute(direct_b, X_AXES, crossed)
    relay_own = step(
        "couple", couple_kernel, shape(2, share, rank), [IN_VMEM] * 2, IN_VMEM, [], 10**7
    )(relay_a, relay_b)
    relays = [lax.ppermute(relay_own, "z", ring(k)) for k in (1, -1, 2)]
    partner_hidden = to_partner(hidden)
    partner_weight = to_partner(down_weight)
    partner_upper = to_partner(up_weight)
    sent = lax.all_to_all(sent, "y", 0, 0, tiled=True)
    leaving = sent[:, 1]

    half = HEAD // 2
    places = (start + jnp.arange(rows, dtype=jnp.int32)).astype(jnp.float32)
    freqs = 10000.0 ** (-2.0 * jnp.arange(half, dtype=jnp.float32) / HEAD)
    angles = places[:, None] * freqs[None, :]
    cosine, sine = jnp.cos(angles), jnp.sin(angles)
    cosine = jnp.where(core == 0, jnp.concatenate([cosine, cosine], axis=1), 1.0)
    sine = jnp.where(core == 0, jnp.concatenate([-sine, sine], axis=1), 0.0)

    flops = 4 * rows * depth * rank2
    partial = step(
        "half",
        half_kernel,
        jax.ShapeDtypeStruct((2 * rows, rank), jnp.float32),
        [IN_SMEM] + [ANYWHERE] * 4,
        IN_VMEM,
        [scratch(2, 2 * rows, depth), scratch(2, depth, rank), sems((6,))],
        flops,
    )(info, hidden, partner_hidden, down_weight, partner_weight)

    latent, pairs = step(
        "project",
        project_kernel,
        (
            pltpu.HBM((2 * rows, rank), jnp.bfloat16),
            pltpu.HBM((2 * groups, rows, HEAD), jnp.bfloat16),
        ),
        [IN_SMEM, IN_VMEM] + [ANYWHERE] * 10 + [IN_VMEM] * 2,
        (ANYWHERE, ANYWHERE),
        [
            scratch(2, 2 * rows, depth),
            scratch(2, depth, rank),
            scratch(rank, kv_width),
            scratch(2 * rows, rank),
            scratch(2 * groups, rows, HEAD),
            sems((20,)),
            sems((2 * groups + 1,)),
        ],
        flops,
    )(
        info, partial, hidden, partner_hidden, direct_a, direct_b,
        relay_own, *relays, up_weight, partner_upper, cosine, sine,
    )

    leaving, pairs = lax.optimization_barrier((leaving, pairs))
    crossed_queries = lax.ppermute(leaving, "xh", [(0, 1), (1, 0)])
    own_pairs = lax.all_to_all(pairs, PLANE + ("core",), 0, 0, tiled=True)
    other_half = to_partner(latent[rows:])

    def part(first, end):
        return own_pairs[2 * first : 2 * end]

    up, down, on = [(0, 1), (1, 2), (2, 3)], [(1, 0), (0, 3)], [(0, 3), (3, 2)]
    passing_2 = lax.ppermute(part(TOP, BLOCKS), "z", down)
    near_low = lax.ppermute(part(0, LOW), "z", up)
    passing_1 = lax.ppermute(part(LOW, TOP), "z", down)
    near_mid = lax.ppermute(part(LOW, MIDDLE), "z", up)
    near_high = lax.ppermute(part(MIDDLE, BLOCKS), "z", up)
    far_low = lax.ppermute(near_low, "z", [(1, 2), (2, 3)])

    common = (info, sent, crossed_queries)
    state = attention_call(own_kernel, 36, (*common, own_pairs), resume=False)
    passing_2, state = lax.optimization_barrier((passing_2, state))
    far_2 = lax.ppermute(passing_2, "z", on)
    state = attention_call(near_kernel, 8 * LOW, (*common, near_low, *state))
    passing_1, state = lax.optimization_barrier((passing_1, state))
    far_1 = lax.ppermute(passing_1, "z", on)
    state = attention_call(near_kernel, 24, (*common, near_mid, *state))
    state = attention_call(near_kernel, 16, (*common, near_high, *state))
    pieces = ((TOP, BLOCKS), (LOW, TOP))
    state = attention_call(
        functools.partial(far_kernel, pieces, False), 30, (*common, far_2, far_1, *state)
    )
    result = attention_call(
        functools.partial(far_kernel, ((0, LOW),), True), 6,
        (*common, far_low, *state), result=True,
    )

    home = lax.all_to_all(result.reshape(groups, rows, PAIR), PLANE, 0, 0, tiled=True)
    each = 2
    attended = pl.pallas_call(
        assemble_kernel,
        out_shape=shape(rows, groups * PAIR),
        grid_spec=pltpu.PrefetchScalarGridSpec(
            num_scalar_prefetch=1,
            grid=(groups // each,),
            in_specs=[pl.BlockSpec((each, rows, PAIR), lambda i, s: (i, 0, 0))],
            out_specs=pl.BlockSpec((rows, each * PAIR), lambda i, s: (0, i)),
        ),
        compiler_params=pltpu.CompilerParams(vmem_limit_bytes=8 * 2**20),
        name="assemble",
    )(info, home)
    live = ((start + jnp.arange(rows, dtype=jnp.int32)) < lengths[0])[:, None]
    ours = latent[:rows]
    both = jnp.where(
        core == 0,
        jnp.concatenate([ours, other_half], axis=1),
        jnp.concatenate([other_half, ours], axis=1),
    )
    latent = jnp.where(live, both, jnp.zeros((), jnp.bfloat16))
    return latent[None], attended[None]


def solution(mesh):
    split = Mesh(mesh.devices.reshape(tuple(SIZES.values())), tuple(SIZES))
    rows = P(DP_AXES, SEQ_AXES, None)
    placed = (rows, rows, P(DP_AXES, None), P(None, DP_AXES, None), P(DP_AXES))

    return jax.shard_map(body, mesh=split, in_specs=placed, out_specs=(rows, rows), check_vma=False)
```

```python
import functools
import itertools

import jax
import jax.numpy as jnp
from jax import lax
from jax.experimental import pallas as pl
from jax.experimental.pallas import tpu as pltpu
from jax.sharding import Mesh
from jax.sharding import PartitionSpec as P


HEAD = 128
PAIR = 2 * HEAD
BLOCK = 256
CHUNK = 2048
KV_HEADS = 8
BLOCKS = CHUNK // BLOCK
LOW = 4
GRANT = {"first": 60, "collect": 60, "gather": 60, "half": 49, "project": 46}
RELAYED = 640
SIZES = {"z": 4, "y": 4, "xh": 2, "xl": 2, "core": 2}
SEQ_AXES = ("z", "y", "xh")
DP_AXES = ("xl", "core")
PLANE = ("y", "xh")

query_scale = 144.0 ** (-0.5)
soft_cap = 50.0
LOG2E = 1.4426950408889634
CONTRACT_LAST = (((1,), (1,)), ((), ()))


X_AXES = ("xh", "xl", "core")


def x_step(flip):
    pairs = []
    for x, core in itertools.product(range(4), range(2)):
        to = (x + (1 if core == 0 else -1)) % 4
        pairs.append((2 * x + core, 2 * to + (core ^ flip)))
    return pairs


def ring(step):
    return [(i, (i + step) % 4) for i in range(4)]


def to_partner(array):
    return lax.ppermute(array, "core", [(0, 1), (1, 0)])


def begin(sems, *moves):
    copies = [pltpu.make_async_copy(a, b, sems.at[k]) for k, (a, b) in enumerate(moves)]
    for copy in copies:
        copy.start()
    return copies


def finish(copies):
    for copy in copies:
        copy.wait()


def chunk(index, size):
    return pl.ds(pl.multiple_of(index * size, size), size)


def first_kernel(info, down, relay_a, relay_b, sems):
    share, rank = relay_a.shape
    split = down.shape[0] - 4 * share
    rows = pl.ds(pl.multiple_of(split + share * info[1], 16), share)
    moves = []
    for flip, relay in ((0, relay_a), (1, relay_b)):
        moves.append((down.at[rows, chunk((info[0] ^ flip) % 2, rank)], relay))
    finish(begin(sems, *moves))


def collect_kernel(info, down, up, direct_a, direct_b, sems):
    rank = direct_a.shape[1]
    piece = up.shape[1]
    split = direct_a.shape[0] - 2 * piece
    moves = []
    for flip, direct in ((0, direct_a), (1, direct_b)):
        which = (info[0] ^ flip) % 2
        columns = chunk(which, rank)
        moves.append((down.at[pl.ds(0, split), columns], direct.at[pl.ds(0, split)]))
        for k in range(2):
            at = pl.ds(split + k * piece, piece)
            moves.append((up.at[which, :, pl.ds(k * rank, rank)], direct.at[at]))
    finish(begin(sems, *moves))


def gather_kernel(info, queries, sent, sems):
    moves = []
    for y, k in itertools.product(range(4), range(2)):
        pair = 2 * y + (info[2] ^ k)
        moves.append((queries.at[:, chunk(pair, PAIR)], sent.at[y, k]))
    finish(begin(sems, *moves))


def couple_kernel(a, b, out):
    out[0] = a[...]
    out[1] = b[...]


def hidden_moves(hidden, partner, shard, into):
    rows = hidden.shape[0]
    columns = chunk(shard, into.shape[1])
    return [
        (hidden.at[:, columns], into.at[pl.ds(0, rows)]),
        (partner.at[:, columns], into.at[pl.ds(rows, rows)]),
    ]


def half_kernel(
    info, hidden, partner, weight_0, weight_1, out, others, inputs, weights, sems
):
    columns = chunk(info[0] % 2, weights.shape[2])
    moves = []
    for k, weight in enumerate((weight_0, weight_1)):
        moves += hidden_moves(hidden, partner, info[0] ^ k, inputs.at[k])
        moves.append((weight.at[:, columns], weights.at[k]))
    for k in range(2):
        moves += hidden_moves(hidden, partner, info[0] ^ (2 + k), others.at[k])
    copies = begin(sems, *moves)
    finish(copies[:3])
    total = jnp.dot(inputs[0], weights[0], preferred_element_type=jnp.float32)
    finish(copies[3:6])
    out[...] = total + jnp.dot(inputs[1], weights[1], preferred_element_type=jnp.float32)
    finish(copies[6:])


def project_kernel(
    info, partial, inputs, direct_a, direct_b, relay_0, relay_1, relay_2, relay_3,
    up_own, up_partner, cosine, sine, latent, pairs,
    weights, upper, rounded, ready, sems, out_sems,
):
    mine, plane = info[0], info[1]
    core = mine % 2
    rows = inputs.shape[1] // 2
    piece = up_own.shape[1]
    share, rank = relay_0.shape[1:]
    split = weights.shape[1] - 4 * share
    moves = []
    for which, direct in ((0, direct_a), (1, direct_b)):
        moves.append((direct.at[pl.ds(0, split)], weights.at[which, pl.ds(0, split)]))
        for step, relay in ((0, relay_0), (3, relay_1), (1, relay_2), (2, relay_3)):
            at = pl.multiple_of(split + share * ((plane + step) % 4), 16)
            moves.append((relay.at[which], weights.at[which, pl.ds(at, share)]))
    count = len(moves) // 2
    moves.append((up_own.at[core], upper.at[chunk(mine, piece)]))
    moves.append((up_partner.at[core], upper.at[chunk(mine ^ 1, piece)]))
    for which, direct in ((0, direct_a), (1, direct_b)):
        for k in range(2):
            at = (chunk(mine ^ (2 + which), piece), pl.ds(k * rank, rank))
            moves.append((direct.at[pl.ds(split + k * piece, piece)], upper.at[at]))
    copies = begin(sems, *moves)
    finish(copies[:count])
    total = partial[...] + jnp.dot(inputs[0], weights[0], preferred_element_type=jnp.float32)
    finish(copies[count : 2 * count])
    total = total + jnp.dot(inputs[1], weights[1], preferred_element_type=jnp.float32)
    rounded[...] = total.astype(jnp.bfloat16)
    outgoing = [pltpu.make_async_copy(rounded, latent, out_sems.at[2 * KV_HEADS])]
    outgoing[0].start()
    finish(copies[2 * count :])
    for head in range(KV_HEADS):
        raw = jnp.dot(
            rounded[...], upper[:, head * HEAD : (head + 1) * HEAD],
            preferred_element_type=jnp.float32,
        )
        for which, turn in ((0, core), (1, 1 - core)):
            entry = raw[which * rows : (which + 1) * rows]
            entry = entry * cosine[...] + pltpu.roll(entry, HEAD // 2, 1) * sine[...]
            ready[2 * head + which] = entry.astype(jnp.bfloat16)
            copy = pltpu.make_async_copy(
                ready.at[2 * head + which],
                pairs.at[2 * head + turn],
                out_sems.at[2 * head + which],
            )
            copy.start()
            outgoing.append(copy)
    finish(outgoing)


def assemble_kernel(info, home, out, masked, sems):
    heads, rows, _ = home.shape
    start, length = info[3], info[4]

    def place(source):
        moves = [(source.at[k], out.at[:, pl.ds(k * PAIR, PAIR)]) for k in range(heads)]
        finish(begin(sems, *moves))

    @pl.when(start + rows <= length)
    def _():
        place(home)

    @pl.when(start + rows > length)
    def _():
        live = (start + lax.broadcasted_iota(jnp.int32, (rows, PAIR), 0)) < length
        for k in range(heads):
            masked[k] = jnp.where(live, home[k], jnp.zeros_like(home[k]))
        place(masked)


def expo(raw):
    return jnp.exp2(jnp.tanh(raw * (query_scale / soft_cap)) * (soft_cap * LOG2E))


def folded(values):
    total = values[:, :HEAD]
    for t in range(1, values.shape[1] // HEAD):
        total = total + values[:, t * HEAD : (t + 1) * HEAD]
    return total


def triangle(newer):
    row = lax.broadcasted_iota(jnp.int32, (2 * BLOCK, BLOCK), 0) % BLOCK
    col = lax.broadcasted_iota(jnp.int32, (2 * BLOCK, BLOCK), 1)
    return col <= row if newer else col > row


def stacked_rows(info, queries, pair, parity):
    kept, crossed = queries
    own = jnp.where(info[2] == parity, kept[pair, 0], crossed[pair])
    return jnp.concatenate([own[:, :HEAD], own[:, HEAD:]], axis=0)


def over_blocks(stacked, pairs, blocks):
    numer = denom = 0.0
    for j, mask in blocks:
        raw = lax.dot_general(
            stacked, pairs[2 * j], CONTRACT_LAST, preferred_element_type=jnp.float32
        )
        e = expo(raw)
        if mask is not None:
            e = jnp.where(mask, e, 0.0)
        denom = denom + folded(e)
        numer = numer + jnp.dot(
            e.astype(jnp.bfloat16), pairs[2 * j + 1], preferred_element_type=jnp.float32
        )
    return numer, denom


def state_rows(i):
    return pl.ds(pl.multiple_of(i * 2 * BLOCK, 2 * BLOCK), 2 * BLOCK)


def own_kernel(info, kept, crossed, pairs, numer, denom):
    mask = triangle(True)
    for i in range(BLOCKS):
        blocks = [(j, None) for j in range(i)] + [(i, mask)]
        numer[state_rows(i), :], denom[state_rows(i), :] = over_blocks(
            stacked_rows(info, (kept, crossed), i // 2, i % 2), pairs, blocks
        )


def two_blocks(info, queries, pair):
    return jnp.concatenate(
        [stacked_rows(info, queries, pair, 0), stacked_rows(info, queries, pair, 1)], axis=0
    )


def pair_rows(pair):
    return chunk(pair, 4 * BLOCK)


def near_kernel(info, kept, crossed, pairs, numer_in, denom_in, numer, denom):
    blocks = [(j, None) for j in range(pairs.shape[0] // 2)]

    @pl.when(info[1] >= 1)
    def _():
        for pair in range(BLOCKS // 2):
            n, d = over_blocks(two_blocks(info, (kept, crossed), pair), pairs, blocks)
            numer[pair_rows(pair), :] += n
            denom[pair_rows(pair), :] += d


def far_kernel(pieces, last, info, kept, crossed, *refs):
    inputs, refs = refs[: len(pieces)], refs[len(pieces) :]
    if last:
        numer, denom, out = refs
    else:
        _, _, numer, denom = refs
    single = triangle(False)
    row = lax.broadcasted_iota(jnp.int32, (4 * BLOCK, BLOCK), 0)
    col = lax.broadcasted_iota(jnp.int32, (4 * BLOCK, BLOCK), 1)
    double = (row < 2 * BLOCK) | (col > row % BLOCK)

    def settle(pair, n, d):
        at = pair_rows(pair)
        if not last:
            numer[at, :], denom[at, :] = n, d
            return
        result = n / jnp.sum(d, axis=1, keepdims=True)
        for k in range(2):
            own = result[2 * k * BLOCK : 2 * (k + 1) * BLOCK]
            out[chunk(2 * pair + k, BLOCK), :] = jnp.concatenate(
                [own[:BLOCK], own[BLOCK:]], axis=1
            ).astype(jnp.bfloat16)

    @pl.when(info[1] >= 2)
    def _():
        for pair in range(BLOCKS // 2):
            i = 2 * pair
            n, d = numer[pair_rows(pair), :], denom[pair_rows(pair), :]
            touched = False
            for ref, (first, end) in zip(inputs, pieces):
                shared = [
                    (j - first, double if j == i + 1 else None)
                    for j in range(max(i + 1, first), end)
                ]
                if shared:
                    more = over_blocks(two_blocks(info, (kept, crossed), pair), ref, shared)
                    n, d, touched = n + more[0], d + more[1], True
                if first <= i < end:
                    own = stacked_rows(info, (kept, crossed), pair, 0)
                    more = over_blocks(own, ref, [(i - first, single)])
                    rest = jnp.zeros((2 * BLOCK, HEAD), jnp.float32)
                    n = n + jnp.concatenate([more[0], rest], axis=0)
                    d = d + jnp.concatenate([more[1], rest], axis=0)
                    touched = True
            if touched or last:
                settle(pair, n, d)

    if last:

        @pl.when(info[1] < 2)
        def _():
            for pair in range(BLOCKS // 2):
                settle(pair, numer[pair_rows(pair), :], denom[pair_rows(pair), :])


IN_VMEM = pl.BlockSpec(memory_space=pltpu.VMEM)
IN_SMEM = pl.BlockSpec(memory_space=pltpu.SMEM)
ANYWHERE = pl.BlockSpec(memory_space=pl.ANY)
STATE = jax.ShapeDtypeStruct((2 * CHUNK, HEAD), jnp.float32)
RESULT = jax.ShapeDtypeStruct((CHUNK, PAIR), jnp.bfloat16)


def attention_call(kernel, count, args, result=False, resume=True):
    single = BLOCK * 2 * BLOCK
    state = len(args) - 2
    return pl.pallas_call(
        kernel,
        out_shape=RESULT if result else (STATE, STATE),
        in_specs=[IN_SMEM] + [IN_VMEM] * (len(args) - 1),
        out_specs=IN_VMEM if result else (IN_VMEM, IN_VMEM),
        input_output_aliases={state: 0, state + 1: 1} if resume and not result else {},
        compiler_params=pltpu.CompilerParams(vmem_limit_bytes=12 * 2**20),
        cost_estimate=pl.CostEstimate(
            flops=count * single * 4 * HEAD, bytes_accessed=2**22, transcendentals=2 * count * single
        ),
    )(*args)


def body(hidden, queries, down_weight, up_weight, lengths):
    _, rows, _ = hidden.shape
    depth, rank2 = down_weight.shape
    rank = rank2 // 2
    piece, kv_width = up_weight.shape[1:]
    groups = kv_width // HEAD
    hidden = hidden[0]
    core = lax.axis_index("core")
    mine = 2 * lax.axis_index("xl") + core
    plane = lax.axis_index("z")
    start = lax.axis_index(SEQ_AXES) * rows
    here = lax.axis_index("xh")
    info = jnp.stack([mine, plane, here, start, lengths[0]]).astype(jnp.int32)

    share = RELAYED // 4
    split = depth - RELAYED
    forward, crossed = x_step(0), x_step(1)

    def shape(*sizes):
        return jax.ShapeDtypeStruct(sizes, jnp.bfloat16)

    def scratch(*sizes):
        return pltpu.VMEM(sizes, jnp.bfloat16)

    def step(name, kernel, out_shape, in_specs, out_specs, scratch_shapes, flops):
        return pl.pallas_call(
            kernel,
            out_shape=out_shape,
            in_specs=in_specs,
            out_specs=out_specs,
            scratch_shapes=scratch_shapes,
            compiler_params=pltpu.CompilerParams(vmem_limit_bytes=GRANT.get(name, 20) * 2**20),
            cost_estimate=pl.CostEstimate(
                flops=flops, bytes_accessed=2**22, transcendentals=0
            ),
        )

    sems = pltpu.SemaphoreType.DMA
    relay_a, relay_b = step(
        "first",
        first_kernel,
        (shape(share, rank),) * 2,
        [IN_SMEM, ANYWHERE],
        (IN_VMEM,) * 2,
        [sems((2,))],
        10**7,
    )(info, down_weight)
    direct_a, direct_b = step(
        "collect",
        collect_kernel,
        (shape(split + 2 * piece, rank),) * 2,
        [IN_SMEM] + [ANYWHERE] * 2,
        (IN_VMEM,) * 2,
        [sems((6,))],
        10**8,
    )(info, down_weight, up_weight)
    relay_a = lax.ppermute(relay_a, X_AXES, forward)
    relay_b = lax.ppermute(relay_b, X_AXES, crossed)
    direct_a = lax.ppermute(direct_a, X_AXES, forward)
    direct_b = lax.ppermute(direct_b, X_AXES, crossed)
    relay_own = step(
        "couple", couple_kernel, shape(2, share, rank), [IN_VMEM] * 2, IN_VMEM, [], 10**7
    )(relay_a, relay_b)
    relays = [lax.ppermute(relay_own, "z", ring(k)) for k in (1, -1, 2)]
    partner_hidden = to_partner(hidden)
    partner_weight = to_partner(down_weight)
    partner_upper = to_partner(up_weight)
    sent = step(
        "gather", gather_kernel, shape(4, 2, rows, PAIR), [IN_SMEM, ANYWHERE], IN_VMEM,
        [sems((8,))], 10**7,
    )(info, queries[0])
    sent = lax.all_to_all(sent, "y", 0, 0, tiled=True)
    leaving = sent[:, 1]

    half = HEAD // 2
    places = (start + jnp.arange(rows, dtype=jnp.int32)).astype(jnp.float32)
    freqs = 10000.0 ** (-2.0 * jnp.arange(half, dtype=jnp.float32) / HEAD)
    angles = places[:, None] * freqs[None, :]
    cosine, sine = jnp.cos(angles), jnp.sin(angles)
    cosine = jnp.where(core == 0, jnp.concatenate([cosine, cosine], axis=1), 1.0)
    sine = jnp.where(core == 0, jnp.concatenate([-sine, sine], axis=1), 0.0)

    flops = 4 * rows * depth * rank2
    partial, others = step(
        "half",
        half_kernel,
        (
            jax.ShapeDtypeStruct((2 * rows, rank), jnp.float32),
            shape(2, 2 * rows, depth),
        ),
        [IN_SMEM] + [ANYWHERE] * 4,
        (IN_VMEM, IN_VMEM),
        [scratch(2, 2 * rows, depth), scratch(2, depth, rank), sems((10,))],
        flops,
    )(info, hidden, partner_hidden, down_weight, partner_weight)

    latent, pairs = step(
        "project",
        project_kernel,
        (
            pltpu.HBM((2 * rows, rank), jnp.bfloat16),
            pltpu.HBM((2 * groups, rows, HEAD), jnp.bfloat16),
        ),
        [IN_SMEM, IN_VMEM, IN_VMEM] + [ANYWHERE] * 8 + [IN_VMEM] * 2,
        (ANYWHERE, ANYWHERE),
        [
            scratch(2, depth, rank),
            scratch(rank, kv_width),
            scratch(2 * rows, rank),
            scratch(2 * groups, rows, HEAD),
            sems((16,)),
            sems((2 * groups + 1,)),
        ],
        flops,
    )(
        info, partial, others, direct_a, direct_b,
        relay_own, *relays, up_weight, partner_upper, cosine, sine,
    )

    leaving, pairs = lax.optimization_barrier((leaving, pairs))
    crossed_queries = lax.ppermute(leaving, "xh", [(0, 1), (1, 0)])
    own_pairs = lax.all_to_all(pairs, PLANE + ("core",), 0, 0, tiled=True)
    other_half = to_partner(latent[rows:])

    low = 2 * LOW
    up, down, on = [(0, 1), (1, 2), (2, 3)], [(1, 0), (0, 3)], [(0, 3), (3, 2)]
    passing = lax.ppermute(own_pairs[low:], "z", down)
    near_low = lax.ppermute(own_pairs[:low], "z", up)
    near_high = lax.ppermute(own_pairs[low:], "z", up)
    far_low = lax.ppermute(near_low, "z", [(1, 2), (2, 3)])

    common = (info, sent, crossed_queries)
    state = attention_call(own_kernel, 36, (*common, own_pairs), resume=False)
    passing, state = lax.optimization_barrier((passing, state))
    far_high = lax.ppermute(passing, "z", on)
    state = attention_call(near_kernel, 32, (*common, near_low, *state))
    state = attention_call(near_kernel, 32, (*common, near_high, *state))
    state = attention_call(
        functools.partial(far_kernel, ((LOW, BLOCKS),), False), 26,
        (*common, far_high, *state),
    )
    result = attention_call(
        functools.partial(far_kernel, ((0, LOW),), True), 10,
        (*common, far_low, *state), result=True,
    )

    home = lax.all_to_all(result.reshape(groups, rows, PAIR), PLANE, 0, 0, tiled=True)
    attended = step(
        "assemble", assemble_kernel, pltpu.HBM((rows, groups * PAIR), jnp.bfloat16),
        [IN_SMEM, IN_VMEM], ANYWHERE, [scratch(groups, rows, PAIR), sems((groups,))], 10**7,
    )(info, home)
    live = ((start + jnp.arange(rows, dtype=jnp.int32)) < lengths[0])[:, None]
    ours = latent[:rows]
    both = jnp.where(
        core == 0,
        jnp.concatenate([ours, other_half], axis=1),
        jnp.concatenate([other_half, ours], axis=1),
    )
    latent = jnp.where(live, both, jnp.zeros((), jnp.bfloat16))
    return latent[None], attended[None]


def solution(mesh):
    split = Mesh(mesh.devices.reshape(tuple(SIZES.values())), tuple(SIZES))
    rows = P(DP_AXES, SEQ_AXES, None)
    placed = (rows, rows, P(DP_AXES, None), P(None, DP_AXES, None), P(DP_AXES))

    return jax.shard_map(body, mesh=split, in_specs=placed, out_specs=(rows, rows), check_vma=False)
```

```python
import functools
import itertools

import jax
import jax.numpy as jnp
from jax import lax
from jax.experimental import pallas as pl
from jax.experimental.pallas import tpu as pltpu
from jax.sharding import Mesh
from jax.sharding import PartitionSpec as P


HEAD = 128
PAIR = 2 * HEAD
BLOCK = 256
CHUNK = 2048
KV_HEADS = 8
BLOCKS = CHUNK // BLOCK
LOW = 4
GRANT = {"first": 60, "collect": 60, "gather": 60, "half": 49, "project": 46}
RELAYED = 640
SIZES = {"z": 4, "y": 4, "xh": 2, "xl": 2, "core": 2}
SEQ_AXES = ("z", "y", "xh")
DP_AXES = ("xl", "core")
PLANE = ("y", "xh")

query_scale = 144.0 ** (-0.5)
soft_cap = 50.0
LOG2E = 1.4426950408889634
CONTRACT_LAST = (((1,), (1,)), ((), ()))


X_AXES = ("xh", "xl", "core")


def x_step(flip):
    pairs = []
    for x, core in itertools.product(range(4), range(2)):
        to = (x + (1 if core == 0 else -1)) % 4
        pairs.append((2 * x + core, 2 * to + (core ^ flip)))
    return pairs


def ring(step):
    return [(i, (i + step) % 4) for i in range(4)]


def to_partner(array):
    return lax.ppermute(array, "core", [(0, 1), (1, 0)])


def begin(sems, *moves):
    copies = [pltpu.make_async_copy(a, b, sems.at[k]) for k, (a, b) in enumerate(moves)]
    for copy in copies:
        copy.start()
    return copies


def finish(copies):
    for copy in copies:
        copy.wait()


def chunk(index, size):
    return pl.ds(pl.multiple_of(index * size, size), size)


def first_kernel(info, down, relay_a, relay_b, sems):
    share, rank = relay_a.shape
    split = down.shape[0] - 4 * share
    rows = pl.ds(pl.multiple_of(split + share * info[1], 16), share)
    moves = []
    for flip, relay in ((0, relay_a), (1, relay_b)):
        moves.append((down.at[rows, chunk((info[0] ^ flip) % 2, rank)], relay))
    finish(begin(sems, *moves))


def collect_kernel(info, down, up, direct_a, direct_b, sems):
    rank = direct_a.shape[1]
    piece = up.shape[1]
    split = direct_a.shape[0] - 2 * piece
    moves = []
    for flip, direct in ((0, direct_a), (1, direct_b)):
        which = (info[0] ^ flip) % 2
        columns = chunk(which, rank)
        moves.append((down.at[pl.ds(0, split), columns], direct.at[pl.ds(0, split)]))
        for k in range(2):
            at = pl.ds(split + k * piece, piece)
            moves.append((up.at[which, :, pl.ds(k * rank, rank)], direct.at[at]))
    finish(begin(sems, *moves))


def gather_kernel(info, queries, sent, sems):
    moves = []
    for y, k in itertools.product(range(4), range(2)):
        pair = 2 * y + (info[2] ^ k)
        moves.append((queries.at[:, chunk(pair, PAIR)], sent.at[y, k]))
    finish(begin(sems, *moves))


def couple_kernel(a, b, out):
    out[0] = a[...]
    out[1] = b[...]


def hidden_moves(hidden, partner, shard, into):
    rows = hidden.shape[0]
    columns = chunk(shard, into.shape[1])
    return [
        (hidden.at[:, columns], into.at[pl.ds(0, rows)]),
        (partner.at[:, columns], into.at[pl.ds(rows, rows)]),
    ]


def half_kernel(
    info, hidden, partner, weight_0, weight_1, out, others, inputs, weights, sems
):
    columns = chunk(info[0] % 2, weights.shape[2])
    moves = []
    for k, weight in enumerate((weight_0, weight_1)):
        moves += hidden_moves(hidden, partner, info[0] ^ k, inputs.at[k])
        moves.append((weight.at[:, columns], weights.at[k]))
    for k in range(2):
        moves += hidden_moves(hidden, partner, info[0] ^ (2 + k), others.at[k])
    copies = begin(sems, *moves)
    finish(copies[:3])
    total = jnp.dot(inputs[0], weights[0], preferred_element_type=jnp.float32)
    finish(copies[3:6])
    out[...] = total + jnp.dot(inputs[1], weights[1], preferred_element_type=jnp.float32)
    finish(copies[6:])


def project_kernel(
    info, partial, inputs, direct_a, direct_b, relay_0, relay_1, relay_2, relay_3,
    up_own, up_partner, cosine, sine, latent, pairs,
    weights, upper, rounded, ready, sems, out_sems,
):
    mine, plane = info[0], info[1]
    core = mine % 2
    rows = inputs.shape[1] // 2
    piece = up_own.shape[1]
    share, rank = relay_0.shape[1:]
    split = weights.shape[1] - 4 * share
    moves = []
    for which, direct in ((0, direct_a), (1, direct_b)):
        moves.append((direct.at[pl.ds(0, split)], weights.at[which, pl.ds(0, split)]))
        for step, relay in ((0, relay_0), (3, relay_1), (1, relay_2), (2, relay_3)):
            at = pl.multiple_of(split + share * ((plane + step) % 4), 16)
            moves.append((relay.at[which], weights.at[which, pl.ds(at, share)]))
    count = len(moves) // 2
    moves.append((up_own.at[core], upper.at[chunk(mine, piece)]))
    moves.append((up_partner.at[core], upper.at[chunk(mine ^ 1, piece)]))
    for which, direct in ((0, direct_a), (1, direct_b)):
        for k in range(2):
            at = (chunk(mine ^ (2 + which), piece), pl.ds(k * rank, rank))
            moves.append((direct.at[pl.ds(split + k * piece, piece)], upper.at[at]))
    copies = begin(sems, *moves)
    finish(copies[:count])
    total = partial[...] + jnp.dot(inputs[0], weights[0], preferred_element_type=jnp.float32)
    finish(copies[count : 2 * count])
    total = total + jnp.dot(inputs[1], weights[1], preferred_element_type=jnp.float32)
    rounded[...] = total.astype(jnp.bfloat16)
    outgoing = [pltpu.make_async_copy(rounded, latent, out_sems.at[2 * KV_HEADS])]
    outgoing[0].start()
    finish(copies[2 * count :])
    for couple in range(KV_HEADS // 2):
        both = jnp.dot(
            rounded[...], upper[:, couple * PAIR : (couple + 1) * PAIR],
            preferred_element_type=jnp.float32,
        )
        for head, (which, turn) in itertools.product(range(2), ((0, core), (1, 1 - core))):
            slot = 2 * (2 * couple + head)
            entry = both[which * rows : (which + 1) * rows, head * HEAD : (head + 1) * HEAD]
            entry = entry * cosine[...] + pltpu.roll(entry, HEAD // 2, 1) * sine[...]
            ready[slot + which] = entry.astype(jnp.bfloat16)
            copy = pltpu.make_async_copy(
                ready.at[slot + which], pairs.at[slot + turn], out_sems.at[slot + which]
            )
            copy.start()
            outgoing.append(copy)
    finish(outgoing)


def assemble_kernel(info, home, out, masked, sems):
    heads, rows, _ = home.shape
    start, length = info[3], info[4]

    def place(source):
        moves = [(source.at[k], out.at[:, pl.ds(k * PAIR, PAIR)]) for k in range(heads)]
        finish(begin(sems, *moves))

    @pl.when(start + rows <= length)
    def _():
        place(home)

    @pl.when(start + rows > length)
    def _():
        live = (start + lax.broadcasted_iota(jnp.int32, (rows, PAIR), 0)) < length
        for k in range(heads):
            masked[k] = jnp.where(live, home[k], jnp.zeros_like(home[k]))
        place(masked)


def expo(raw):
    return jnp.exp2(jnp.tanh(raw * (query_scale / soft_cap)) * (soft_cap * LOG2E))


def folded(values):
    total = values[:, :HEAD]
    for t in range(1, values.shape[1] // HEAD):
        total = total + values[:, t * HEAD : (t + 1) * HEAD]
    return total


def triangle(newer):
    row = lax.broadcasted_iota(jnp.int32, (2 * BLOCK, BLOCK), 0) % BLOCK
    col = lax.broadcasted_iota(jnp.int32, (2 * BLOCK, BLOCK), 1)
    return col <= row if newer else col > row


def stacked_rows(info, queries, pair, parity):
    kept, crossed = queries
    own = jnp.where(info[2] == parity, kept[pair, 0], crossed[pair])
    return jnp.concatenate([own[:, :HEAD], own[:, HEAD:]], axis=0)


def over_blocks(stacked, pairs, blocks):
    numer = denom = 0.0
    for j, mask in blocks:
        raw = lax.dot_general(
            stacked, pairs[2 * j], CONTRACT_LAST, preferred_element_type=jnp.float32
        )
        e = expo(raw)
        if mask is not None:
            e = jnp.where(mask, e, 0.0)
        denom = denom + folded(e)
        numer = numer + jnp.dot(
            e.astype(jnp.bfloat16), pairs[2 * j + 1], preferred_element_type=jnp.float32
        )
    return numer, denom


def state_rows(i):
    return pl.ds(pl.multiple_of(i * 2 * BLOCK, 2 * BLOCK), 2 * BLOCK)


def own_kernel(info, kept, crossed, pairs, numer, denom):
    mask = triangle(True)
    for i in range(BLOCKS):
        blocks = [(j, None) for j in range(i)] + [(i, mask)]
        numer[state_rows(i), :], denom[state_rows(i), :] = over_blocks(
            stacked_rows(info, (kept, crossed), i // 2, i % 2), pairs, blocks
        )


def two_blocks(info, queries, pair):
    return jnp.concatenate(
        [stacked_rows(info, queries, pair, 0), stacked_rows(info, queries, pair, 1)], axis=0
    )


def pair_rows(pair):
    return chunk(pair, 4 * BLOCK)


def near_kernel(info, kept, crossed, pairs, numer_in, denom_in, numer, denom):
    blocks = [(j, None) for j in range(pairs.shape[0] // 2)]

    @pl.when(info[1] >= 1)
    def _():
        for pair in range(BLOCKS // 2):
            n, d = over_blocks(two_blocks(info, (kept, crossed), pair), pairs, blocks)
            numer[pair_rows(pair), :] += n
            denom[pair_rows(pair), :] += d


def far_kernel(pieces, info, kept, crossed, *refs):
    inputs, (numer, denom, out) = refs[: len(pieces)], refs[len(pieces) :]
    single = triangle(False)
    row = lax.broadcasted_iota(jnp.int32, (4 * BLOCK, BLOCK), 0)
    col = lax.broadcasted_iota(jnp.int32, (4 * BLOCK, BLOCK), 1)
    double = (row < 2 * BLOCK) | (col > row % BLOCK)

    def settle(pair, n, d):
        result = n / jnp.sum(d, axis=1, keepdims=True)
        for k in range(2):
            own = result[2 * k * BLOCK : 2 * (k + 1) * BLOCK]
            out[chunk(2 * pair + k, BLOCK), :] = jnp.concatenate(
                [own[:BLOCK], own[BLOCK:]], axis=1
            ).astype(jnp.bfloat16)

    @pl.when(info[1] >= 2)
    def _():
        for pair in range(BLOCKS // 2):
            i = 2 * pair
            n, d = numer[pair_rows(pair), :], denom[pair_rows(pair), :]
            for ref, (first, end) in zip(inputs, pieces):
                shared = [
                    (j - first, double if j == i + 1 else None)
                    for j in range(max(i + 1, first), end)
                ]
                if shared:
                    more = over_blocks(two_blocks(info, (kept, crossed), pair), ref, shared)
                    n, d = n + more[0], d + more[1]
                if first <= i < end:
                    own = stacked_rows(info, (kept, crossed), pair, 0)
                    more = over_blocks(own, ref, [(i - first, single)])
                    rest = jnp.zeros((2 * BLOCK, HEAD), jnp.float32)
                    n = n + jnp.concatenate([more[0], rest], axis=0)
                    d = d + jnp.concatenate([more[1], rest], axis=0)
            settle(pair, n, d)

    @pl.when(info[1] < 2)
    def _():
        for pair in range(BLOCKS // 2):
            settle(pair, numer[pair_rows(pair), :], denom[pair_rows(pair), :])


IN_VMEM = pl.BlockSpec(memory_space=pltpu.VMEM)
IN_SMEM = pl.BlockSpec(memory_space=pltpu.SMEM)
ANYWHERE = pl.BlockSpec(memory_space=pl.ANY)
STATE = jax.ShapeDtypeStruct((2 * CHUNK, HEAD), jnp.float32)
RESULT = jax.ShapeDtypeStruct((CHUNK, PAIR), jnp.bfloat16)


def attention_call(kernel, count, args, result=False, resume=True):
    single = BLOCK * 2 * BLOCK
    state = len(args) - 2
    return pl.pallas_call(
        kernel,
        out_shape=RESULT if result else (STATE, STATE),
        in_specs=[IN_SMEM] + [IN_VMEM] * (len(args) - 1),
        out_specs=IN_VMEM if result else (IN_VMEM, IN_VMEM),
        input_output_aliases={state: 0, state + 1: 1} if resume and not result else {},
        compiler_params=pltpu.CompilerParams(vmem_limit_bytes=12 * 2**20),
        cost_estimate=pl.CostEstimate(
            flops=count * single * 4 * HEAD, bytes_accessed=2**22, transcendentals=2 * count * single
        ),
    )(*args)


def body(hidden, queries, down_weight, up_weight, lengths):
    _, rows, _ = hidden.shape
    depth, rank2 = down_weight.shape
    rank = rank2 // 2
    piece, kv_width = up_weight.shape[1:]
    groups = kv_width // HEAD
    hidden = hidden[0]
    core = lax.axis_index("core")
    mine = 2 * lax.axis_index("xl") + core
    plane = lax.axis_index("z")
    start = lax.axis_index(SEQ_AXES) * rows
    here = lax.axis_index("xh")
    info = jnp.stack([mine, plane, here, start, lengths[0]]).astype(jnp.int32)

    share = RELAYED // 4
    split = depth - RELAYED
    forward, crossed = x_step(0), x_step(1)

    def shape(*sizes):
        return jax.ShapeDtypeStruct(sizes, jnp.bfloat16)

    def scratch(*sizes):
        return pltpu.VMEM(sizes, jnp.bfloat16)

    def step(name, kernel, out_shape, in_specs, out_specs, scratch_shapes, flops):
        return pl.pallas_call(
            kernel,
            out_shape=out_shape,
            in_specs=in_specs,
            out_specs=out_specs,
            scratch_shapes=scratch_shapes,
            compiler_params=pltpu.CompilerParams(vmem_limit_bytes=GRANT.get(name, 20) * 2**20),
            cost_estimate=pl.CostEstimate(
                flops=flops, bytes_accessed=2**22, transcendentals=0
            ),
        )

    sems = pltpu.SemaphoreType.DMA
    relay_a, relay_b = step(
        "first",
        first_kernel,
        (shape(share, rank),) * 2,
        [IN_SMEM, ANYWHERE],
        (IN_VMEM,) * 2,
        [sems((2,))],
        10**7,
    )(info, down_weight)
    direct_a, direct_b = step(
        "collect",
        collect_kernel,
        (shape(split + 2 * piece, rank),) * 2,
        [IN_SMEM] + [ANYWHERE] * 2,
        (IN_VMEM,) * 2,
        [sems((6,))],
        10**8,
    )(info, down_weight, up_weight)
    relay_a = lax.ppermute(relay_a, X_AXES, forward)
    relay_b = lax.ppermute(relay_b, X_AXES, crossed)
    direct_a = lax.ppermute(direct_a, X_AXES, forward)
    direct_b = lax.ppermute(direct_b, X_AXES, crossed)
    relay_own = step(
        "couple", couple_kernel, shape(2, share, rank), [IN_VMEM] * 2, IN_VMEM, [], 10**7
    )(relay_a, relay_b)
    relays = [lax.ppermute(relay_own, "z", ring(k)) for k in (1, -1, 2)]
    partner_hidden = to_partner(hidden)
    partner_weight = to_partner(down_weight)
    partner_upper = to_partner(up_weight)
    sent = step(
        "gather", gather_kernel, shape(4, 2, rows, PAIR), [IN_SMEM, ANYWHERE], IN_VMEM,
        [sems((8,))], 10**7,
    )(info, queries[0])
    sent = lax.all_to_all(sent, "y", 0, 0, tiled=True)
    leaving = sent[:, 1]

    half = HEAD // 2
    places = (start + jnp.arange(rows, dtype=jnp.int32)).astype(jnp.float32)
    freqs = 10000.0 ** (-2.0 * jnp.arange(half, dtype=jnp.float32) / HEAD)
    angles = places[:, None] * freqs[None, :]
    cosine, sine = jnp.cos(angles), jnp.sin(angles)
    cosine = jnp.where(core == 0, jnp.concatenate([cosine, cosine], axis=1), 1.0)
    sine = jnp.where(core == 0, jnp.concatenate([-sine, sine], axis=1), 0.0)

    flops = 4 * rows * depth * rank2
    partial, others = step(
        "half",
        half_kernel,
        (
            jax.ShapeDtypeStruct((2 * rows, rank), jnp.float32),
            shape(2, 2 * rows, depth),
        ),
        [IN_SMEM] + [ANYWHERE] * 4,
        (IN_VMEM, IN_VMEM),
        [scratch(2, 2 * rows, depth), scratch(2, depth, rank), sems((10,))],
        flops,
    )(info, hidden, partner_hidden, down_weight, partner_weight)

    latent, pairs = step(
        "project",
        project_kernel,
        (
            pltpu.HBM((2 * rows, rank), jnp.bfloat16),
            pltpu.HBM((2 * groups, rows, HEAD), jnp.bfloat16),
        ),
        [IN_SMEM, IN_VMEM, IN_VMEM] + [ANYWHERE] * 8 + [IN_VMEM] * 2,
        (ANYWHERE, ANYWHERE),
        [
            scratch(2, depth, rank),
            scratch(rank, kv_width),
            scratch(2 * rows, rank),
            scratch(2 * groups, rows, HEAD),
            sems((16,)),
            sems((2 * groups + 1,)),
        ],
        flops,
    )(
        info, partial, others, direct_a, direct_b,
        relay_own, *relays, up_weight, partner_upper, cosine, sine,
    )

    leaving, pairs = lax.optimization_barrier((leaving, pairs))
    crossed_queries = lax.ppermute(leaving, "xh", [(0, 1), (1, 0)])
    own_pairs = lax.all_to_all(pairs, PLANE + ("core",), 0, 0, tiled=True)
    other_half = to_partner(latent[rows:])

    low = 2 * LOW
    up, down, on = [(0, 1), (1, 2), (2, 3)], [(1, 0), (0, 3)], [(0, 3), (3, 2)]
    passing = lax.ppermute(own_pairs[low:], "z", down)
    near_low = lax.ppermute(own_pairs[:low], "z", up)
    near_high = lax.ppermute(own_pairs[low:], "z", up)
    far_low = lax.ppermute(near_low, "z", [(1, 2), (2, 3)])

    common = (info, sent, crossed_queries)
    state = attention_call(own_kernel, 36, (*common, own_pairs), resume=False)
    passing, state = lax.optimization_barrier((passing, state))
    far_high = lax.ppermute(passing, "z", on)
    state = attention_call(near_kernel, 32, (*common, near_low, *state))
    state = attention_call(near_kernel, 32, (*common, near_high, *state))
    result = attention_call(
        functools.partial(far_kernel, ((LOW, BLOCKS), (0, LOW))), 36,
        (*common, far_high, far_low, *state), result=True,
    )

    home = lax.all_to_all(result.reshape(groups, rows, PAIR), PLANE, 0, 0, tiled=True)
    attended = step(
        "assemble", assemble_kernel, pltpu.HBM((rows, groups * PAIR), jnp.bfloat16),
        [IN_SMEM, IN_VMEM], ANYWHERE, [scratch(groups, rows, PAIR), sems((groups,))], 10**7,
    )(info, home)
    live = ((start + jnp.arange(rows, dtype=jnp.int32)) < lengths[0])[:, None]
    ours = latent[:rows]
    both = jnp.where(
        core == 0,
        jnp.concatenate([ours, other_half], axis=1),
        jnp.concatenate([other_half, ours], axis=1),
    )
    latent = jnp.where(live, both, jnp.zeros((), jnp.bfloat16))
    return latent[None], attended[None]


def solution(mesh):
    split = Mesh(mesh.devices.reshape(tuple(SIZES.values())), tuple(SIZES))
    rows = P(DP_AXES, SEQ_AXES, None)
    placed = (rows, rows, P(DP_AXES, None), P(None, DP_AXES, None), P(DP_AXES))

    return jax.shard_map(body, mesh=split, in_specs=placed, out_specs=(rows, rows), check_vma=False)
```

```python
import functools
import itertools

import jax
import jax.numpy as jnp
from jax import lax
from jax.experimental import pallas as pl
from jax.experimental.pallas import tpu as pltpu
from jax.sharding import Mesh
from jax.sharding import PartitionSpec as P


HEAD = 128
PAIR = 2 * HEAD
BLOCK = 256
CHUNK = 2048
KV_HEADS = 8
BLOCKS = CHUNK // BLOCK
LOW = 4
GRANT = {"first": 60, "collect": 60, "half": 49, "project": 46}
RELAYED = 640
SIZES = {"z": 4, "y": 4, "xh": 2, "xl": 2, "core": 2}
SEQ_AXES = ("z", "y", "xh")
DP_AXES = ("xl", "core")
PLANE = ("y", "xh")

query_scale = 144.0 ** (-0.5)
soft_cap = 50.0
LOG2E = 1.4426950408889634
CONTRACT_LAST = (((1,), (1,)), ((), ()))


X_AXES = ("xh", "xl", "core")


def x_step(flip):
    pairs = []
    for x, core in itertools.product(range(4), range(2)):
        to = (x + (1 if core == 0 else -1)) % 4
        pairs.append((2 * x + core, 2 * to + (core ^ flip)))
    return pairs


def ring(step):
    return [(i, (i + step) % 4) for i in range(4)]


def to_partner(array):
    return lax.ppermute(array, "core", [(0, 1), (1, 0)])


def begin(sems, *moves):
    copies = [pltpu.make_async_copy(a, b, sems.at[k]) for k, (a, b) in enumerate(moves)]
    for copy in copies:
        copy.start()
    return copies


def finish(copies):
    for copy in copies:
        copy.wait()


def chunk(index, size):
    return pl.ds(pl.multiple_of(index * size, size), size)


def first_kernel(info, down, relay_a, relay_b, sems):
    share, rank = relay_a.shape
    split = down.shape[0] - 4 * share
    rows = pl.ds(pl.multiple_of(split + share * info[1], 16), share)
    moves = []
    for flip, relay in ((0, relay_a), (1, relay_b)):
        moves.append((down.at[rows, chunk((info[0] ^ flip) % 2, rank)], relay))
    finish(begin(sems, *moves))


def collect_kernel(info, down, up, queries, direct_a, direct_b, sent, sems):
    rank = direct_a.shape[1]
    piece = up.shape[1]
    split = direct_a.shape[0] - 2 * piece
    moves = []
    for flip, direct in ((0, direct_a), (1, direct_b)):
        which = (info[0] ^ flip) % 2
        columns = chunk(which, rank)
        moves.append((down.at[pl.ds(0, split), columns], direct.at[pl.ds(0, split)]))
        for k in range(2):
            at = pl.ds(split + k * piece, piece)
            moves.append((up.at[which, :, pl.ds(k * rank, rank)], direct.at[at]))
    for y, k in itertools.product(range(4), range(2)):
        pair = 2 * y + (info[2] ^ k)
        moves.append((queries.at[:, chunk(pair, PAIR)], sent.at[y, k]))
    finish(begin(sems, *moves))


def couple_kernel(a, b, out):
    out[0] = a[...]
    out[1] = b[...]


def hidden_moves(hidden, partner, shard, into):
    rows = hidden.shape[0]
    columns = chunk(shard, into.shape[1])
    return [
        (hidden.at[:, columns], into.at[pl.ds(0, rows)]),
        (partner.at[:, columns], into.at[pl.ds(rows, rows)]),
    ]


def half_kernel(
    info, hidden, partner, weight_0, weight_1, out, others, inputs, weights, sems
):
    columns = chunk(info[0] % 2, weights.shape[2])
    moves = []
    for k, weight in enumerate((weight_0, weight_1)):
        moves += hidden_moves(hidden, partner, info[0] ^ k, inputs.at[k])
        moves.append((weight.at[:, columns], weights.at[k]))
    for k in range(2):
        moves += hidden_moves(hidden, partner, info[0] ^ (2 + k), others.at[k])
    copies = begin(sems, *moves)
    finish(copies[:3])
    total = jnp.dot(inputs[0], weights[0], preferred_element_type=jnp.float32)
    finish(copies[3:6])
    out[...] = total + jnp.dot(inputs[1], weights[1], preferred_element_type=jnp.float32)
    finish(copies[6:])


def project_kernel(
    info, partial, inputs, direct_a, direct_b, relay_0, relay_1, relay_2, relay_3,
    up_own, up_partner, cosine, sine, latent, pairs,
    weights, upper, rounded, ready, sems, out_sems,
):
    mine, plane = info[0], info[1]
    core = mine % 2
    rows = inputs.shape[1] // 2
    piece = up_own.shape[1]
    share, rank = relay_0.shape[1:]
    split = weights.shape[1] - 4 * share
    moves = []
    for which, direct in ((0, direct_a), (1, direct_b)):
        moves.append((direct.at[pl.ds(0, split)], weights.at[which, pl.ds(0, split)]))
        for step, relay in ((0, relay_0), (3, relay_1), (1, relay_2), (2, relay_3)):
            at = pl.multiple_of(split + share * ((plane + step) % 4), 16)
            moves.append((relay.at[which], weights.at[which, pl.ds(at, share)]))
    count = len(moves) // 2
    moves.append((up_own.at[core], upper.at[chunk(mine, piece)]))
    moves.append((up_partner.at[core], upper.at[chunk(mine ^ 1, piece)]))
    for which, direct in ((0, direct_a), (1, direct_b)):
        for k in range(2):
            at = (chunk(mine ^ (2 + which), piece), pl.ds(k * rank, rank))
            moves.append((direct.at[pl.ds(split + k * piece, piece)], upper.at[at]))
    copies = begin(sems, *moves)
    finish(copies[:count])
    total = partial[...] + jnp.dot(inputs[0], weights[0], preferred_element_type=jnp.float32)
    finish(copies[count : 2 * count])
    total = total + jnp.dot(inputs[1], weights[1], preferred_element_type=jnp.float32)
    rounded[...] = total.astype(jnp.bfloat16)
    outgoing = [pltpu.make_async_copy(rounded, latent, out_sems.at[2 * KV_HEADS])]
    outgoing[0].start()
    finish(copies[2 * count :])
    for couple in range(KV_HEADS // 2):
        both = jnp.dot(
            rounded[...], upper[:, couple * PAIR : (couple + 1) * PAIR],
            preferred_element_type=jnp.float32,
        )
        for head, (which, turn) in itertools.product(range(2), ((0, core), (1, 1 - core))):
            slot = 2 * (2 * couple + head)
            entry = both[which * rows : (which + 1) * rows, head * HEAD : (head + 1) * HEAD]
            entry = entry * cosine[...] + pltpu.roll(entry, HEAD // 2, 1) * sine[...]
            ready[slot + which] = entry.astype(jnp.bfloat16)
            copy = pltpu.make_async_copy(
                ready.at[slot + which], pairs.at[slot + turn], out_sems.at[slot + which]
            )
            copy.start()
            outgoing.append(copy)
    finish(outgoing)


def assemble_kernel(info, home, out, masked, sems):
    heads, rows, _ = home.shape
    start, length = info[3], info[4]

    def place(source):
        moves = [(source.at[k], out.at[:, pl.ds(k * PAIR, PAIR)]) for k in range(heads)]
        finish(begin(sems, *moves))

    @pl.when(start + rows <= length)
    def _():
        place(home)

    @pl.when(start + rows > length)
    def _():
        live = (start + lax.broadcasted_iota(jnp.int32, (rows, PAIR), 0)) < length
        for k in range(heads):
            masked[k] = jnp.where(live, home[k], jnp.zeros_like(home[k]))
        place(masked)


def expo(raw):
    return jnp.exp2(jnp.tanh(raw * (query_scale / soft_cap)) * (soft_cap * LOG2E))


def folded(values):
    total = values[:, :HEAD]
    for t in range(1, values.shape[1] // HEAD):
        total = total + values[:, t * HEAD : (t + 1) * HEAD]
    return total


def triangle(newer):
    row = lax.broadcasted_iota(jnp.int32, (2 * BLOCK, BLOCK), 0) % BLOCK
    col = lax.broadcasted_iota(jnp.int32, (2 * BLOCK, BLOCK), 1)
    return col <= row if newer else col > row


def stacked_rows(info, queries, pair, parity):
    kept, crossed = queries
    own = jnp.where(info[2] == parity, kept[pair, 0], crossed[pair])
    return jnp.concatenate([own[:, :HEAD], own[:, HEAD:]], axis=0)


def over_blocks(stacked, pairs, blocks):
    numer = denom = 0.0
    for j, mask in blocks:
        raw = lax.dot_general(
            stacked, pairs[2 * j], CONTRACT_LAST, preferred_element_type=jnp.float32
        )
        e = expo(raw)
        if mask is not None:
            e = jnp.where(mask, e, 0.0)
        denom = denom + folded(e)
        numer = numer + jnp.dot(
            e.astype(jnp.bfloat16), pairs[2 * j + 1], preferred_element_type=jnp.float32
        )
    return numer, denom


def state_rows(i):
    return pl.ds(pl.multiple_of(i * 2 * BLOCK, 2 * BLOCK), 2 * BLOCK)


def own_kernel(info, kept, crossed, pairs, numer, denom):
    mask = triangle(True)
    for i in range(BLOCKS):
        blocks = [(j, None) for j in range(i)] + [(i, mask)]
        numer[state_rows(i), :], denom[state_rows(i), :] = over_blocks(
            stacked_rows(info, (kept, crossed), i // 2, i % 2), pairs, blocks
        )


def two_blocks(info, queries, pair):
    return jnp.concatenate(
        [stacked_rows(info, queries, pair, 0), stacked_rows(info, queries, pair, 1)], axis=0
    )


def pair_rows(pair):
    return chunk(pair, 4 * BLOCK)


def near_kernel(info, kept, crossed, pairs, numer_in, denom_in, numer, denom):
    blocks = [(j, None) for j in range(pairs.shape[0] // 2)]

    @pl.when(info[1] >= 1)
    def _():
        for pair in range(BLOCKS // 2):
            n, d = over_blocks(two_blocks(info, (kept, crossed), pair), pairs, blocks)
            numer[pair_rows(pair), :] += n
            denom[pair_rows(pair), :] += d


def far_kernel(pieces, last, info, kept, crossed, *refs):
    inputs, refs = refs[: len(pieces)], refs[len(pieces) :]
    if last:
        numer, denom, out = refs
    else:
        _, _, numer, denom = refs
    single = triangle(False)
    row = lax.broadcasted_iota(jnp.int32, (4 * BLOCK, BLOCK), 0)
    col = lax.broadcasted_iota(jnp.int32, (4 * BLOCK, BLOCK), 1)
    double = (row < 2 * BLOCK) | (col > row % BLOCK)

    def settle(pair, n, d):
        at = pair_rows(pair)
        if not last:
            numer[at, :], denom[at, :] = n, d
            return
        result = n / jnp.sum(d, axis=1, keepdims=True)
        for k in range(2):
            own = result[2 * k * BLOCK : 2 * (k + 1) * BLOCK]
            out[chunk(2 * pair + k, BLOCK), :] = jnp.concatenate(
                [own[:BLOCK], own[BLOCK:]], axis=1
            ).astype(jnp.bfloat16)

    @pl.when(info[1] >= 2)
    def _():
        for pair in range(BLOCKS // 2):
            i = 2 * pair
            n, d = numer[pair_rows(pair), :], denom[pair_rows(pair), :]
            touched = False
            for ref, (first, end) in zip(inputs, pieces):
                shared = [
                    (j - first, double if j == i + 1 else None)
                    for j in range(max(i + 1, first), end)
                ]
                if shared:
                    more = over_blocks(two_blocks(info, (kept, crossed), pair), ref, shared)
                    n, d, touched = n + more[0], d + more[1], True
                if first <= i < end:
                    own = stacked_rows(info, (kept, crossed), pair, 0)
                    more = over_blocks(own, ref, [(i - first, single)])
                    rest = jnp.zeros((2 * BLOCK, HEAD), jnp.float32)
                    n = n + jnp.concatenate([more[0], rest], axis=0)
                    d = d + jnp.concatenate([more[1], rest], axis=0)
                    touched = True
            if touched or last:
                settle(pair, n, d)

    if last:

        @pl.when(info[1] < 2)
        def _():
            for pair in range(BLOCKS // 2):
                settle(pair, numer[pair_rows(pair), :], denom[pair_rows(pair), :])


IN_VMEM = pl.BlockSpec(memory_space=pltpu.VMEM)
IN_SMEM = pl.BlockSpec(memory_space=pltpu.SMEM)
ANYWHERE = pl.BlockSpec(memory_space=pl.ANY)
STATE = jax.ShapeDtypeStruct((2 * CHUNK, HEAD), jnp.float32)
RESULT = jax.ShapeDtypeStruct((CHUNK, PAIR), jnp.bfloat16)


def attention_call(kernel, count, args, result=False, resume=True):
    single = BLOCK * 2 * BLOCK
    state = len(args) - 2
    return pl.pallas_call(
        kernel,
        out_shape=RESULT if result else (STATE, STATE),
        in_specs=[IN_SMEM] + [IN_VMEM] * (len(args) - 1),
        out_specs=IN_VMEM if result else (IN_VMEM, IN_VMEM),
        input_output_aliases={state: 0, state + 1: 1} if resume and not result else {},
        compiler_params=pltpu.CompilerParams(vmem_limit_bytes=12 * 2**20),
        cost_estimate=pl.CostEstimate(
            flops=count * single * 4 * HEAD, bytes_accessed=2**22, transcendentals=2 * count * single
        ),
    )(*args)


def body(hidden, queries, down_weight, up_weight, lengths):
    _, rows, _ = hidden.shape
    depth, rank2 = down_weight.shape
    rank = rank2 // 2
    piece, kv_width = up_weight.shape[1:]
    groups = kv_width // HEAD
    hidden = hidden[0]
    core = lax.axis_index("core")
    mine = 2 * lax.axis_index("xl") + core
    plane = lax.axis_index("z")
    start = lax.axis_index(SEQ_AXES) * rows
    here = lax.axis_index("xh")
    info = jnp.stack([mine, plane, here, start, lengths[0]]).astype(jnp.int32)

    share = RELAYED // 4
    split = depth - RELAYED
    forward, crossed = x_step(0), x_step(1)

    def shape(*sizes):
        return jax.ShapeDtypeStruct(sizes, jnp.bfloat16)

    def scratch(*sizes):
        return pltpu.VMEM(sizes, jnp.bfloat16)

    def step(name, kernel, out_shape, in_specs, out_specs, scratch_shapes, flops):
        return pl.pallas_call(
            kernel,
            out_shape=out_shape,
            in_specs=in_specs,
            out_specs=out_specs,
            scratch_shapes=scratch_shapes,
            compiler_params=pltpu.CompilerParams(vmem_limit_bytes=GRANT.get(name, 20) * 2**20),
            cost_estimate=pl.CostEstimate(
                flops=flops, bytes_accessed=2**22, transcendentals=0
            ),
        )

    sems = pltpu.SemaphoreType.DMA
    relay_a, relay_b = step(
        "first",
        first_kernel,
        (shape(share, rank),) * 2,
        [IN_SMEM, ANYWHERE],
        (IN_VMEM,) * 2,
        [sems((2,))],
        10**7,
    )(info, down_weight)
    direct_a, direct_b, sent = step(
        "collect",
        collect_kernel,
        (shape(split + 2 * piece, rank),) * 2 + (shape(4, 2, rows, PAIR),),
        [IN_SMEM] + [ANYWHERE] * 3,
        (IN_VMEM,) * 3,
        [sems((14,))],
        10**8,
    )(info, down_weight, up_weight, queries[0])
    relay_a = lax.ppermute(relay_a, X_AXES, forward)
    relay_b = lax.ppermute(relay_b, X_AXES, crossed)
    direct_a = lax.ppermute(direct_a, X_AXES, forward)
    direct_b = lax.ppermute(direct_b, X_AXES, crossed)
    relay_own = step(
        "couple", couple_kernel, shape(2, share, rank), [IN_VMEM] * 2, IN_VMEM, [], 10**7
    )(relay_a, relay_b)
    relays = [lax.ppermute(relay_own, "z", ring(k)) for k in (1, -1, 2)]
    partner_hidden = to_partner(hidden)
    partner_weight = to_partner(down_weight)
    partner_upper = to_partner(up_weight)
    sent = lax.all_to_all(sent, "y", 0, 0, tiled=True)
    leaving = sent[:, 1]

    half = HEAD // 2
    places = (start + jnp.arange(rows, dtype=jnp.int32)).astype(jnp.float32)
    freqs = 10000.0 ** (-2.0 * jnp.arange(half, dtype=jnp.float32) / HEAD)
    angles = places[:, None] * freqs[None, :]
    cosine, sine = jnp.cos(angles), jnp.sin(angles)
    cosine = jnp.where(core == 0, jnp.concatenate([cosine, cosine], axis=1), 1.0)
    sine = jnp.where(core == 0, jnp.concatenate([-sine, sine], axis=1), 0.0)

    flops = 4 * rows * depth * rank2
    partial, others = step(
        "half",
        half_kernel,
        (
            jax.ShapeDtypeStruct((2 * rows, rank), jnp.float32),
            shape(2, 2 * rows, depth),
        ),
        [IN_SMEM] + [ANYWHERE] * 4,
        (IN_VMEM, IN_VMEM),
        [scratch(2, 2 * rows, depth), scratch(2, depth, rank), sems((10,))],
        flops,
    )(info, hidden, partner_hidden, down_weight, partner_weight)

    latent, pairs = step(
        "project",
        project_kernel,
        (
            pltpu.HBM((2 * rows, rank), jnp.bfloat16),
            pltpu.HBM((2 * groups, rows, HEAD), jnp.bfloat16),
        ),
        [IN_SMEM, IN_VMEM, IN_VMEM] + [ANYWHERE] * 8 + [IN_VMEM] * 2,
        (ANYWHERE, ANYWHERE),
        [
            scratch(2, depth, rank),
            scratch(rank, kv_width),
            scratch(2 * rows, rank),
            scratch(2 * groups, rows, HEAD),
            sems((16,)),
            sems((2 * groups + 1,)),
        ],
        flops,
    )(
        info, partial, others, direct_a, direct_b,
        relay_own, *relays, up_weight, partner_upper, cosine, sine,
    )

    leaving, pairs = lax.optimization_barrier((leaving, pairs))
    crossed_queries = lax.ppermute(leaving, "xh", [(0, 1), (1, 0)])
    own_pairs = lax.all_to_all(pairs, PLANE + ("core",), 0, 0, tiled=True)
    other_half = to_partner(latent[rows:])

    low = 2 * LOW
    up, down, on = [(0, 1), (1, 2), (2, 3)], [(1, 0), (0, 3)], [(0, 3), (3, 2)]
    passing = lax.ppermute(own_pairs[low:], "z", down)
    near_low = lax.ppermute(own_pairs[:low], "z", up)
    near_high = lax.ppermute(own_pairs[low:], "z", up)
    far_low = lax.ppermute(near_low, "z", [(1, 2), (2, 3)])

    common = (info, sent, crossed_queries)
    state = attention_call(own_kernel, 36, (*common, own_pairs), resume=False)
    passing, state = lax.optimization_barrier((passing, state))
    far_high = lax.ppermute(passing, "z", on)
    state = attention_call(near_kernel, 32, (*common, near_low, *state))
    state = attention_call(near_kernel, 32, (*common, near_high, *state))
    state = attention_call(
        functools.partial(far_kernel, ((LOW, BLOCKS),), False), 26,
        (*common, far_high, *state),
    )
    result = attention_call(
        functools.partial(far_kernel, ((0, LOW),), True), 10,
        (*common, far_low, *state), result=True,
    )

    home = lax.all_to_all(result.reshape(groups, rows, PAIR), PLANE, 0, 0, tiled=True)
    attended = step(
        "assemble", assemble_kernel, pltpu.HBM((rows, groups * PAIR), jnp.bfloat16),
        [IN_SMEM, IN_VMEM], ANYWHERE, [scratch(groups, rows, PAIR), sems((groups,))], 10**7,
    )(info, home)
    live = ((start + jnp.arange(rows, dtype=jnp.int32)) < lengths[0])[:, None]
    ours = latent[:rows]
    both = jnp.where(
        core == 0,
        jnp.concatenate([ours, other_half], axis=1),
        jnp.concatenate([other_half, ours], axis=1),
    )
    latent = jnp.where(live, both, jnp.zeros((), jnp.bfloat16))
    return latent[None], attended[None]


def solution(mesh):
    split = Mesh(mesh.devices.reshape(tuple(SIZES.values())), tuple(SIZES))
    rows = P(DP_AXES, SEQ_AXES, None)
    placed = (rows, rows, P(DP_AXES, None), P(None, DP_AXES, None), P(DP_AXES))

    return jax.shard_map(body, mesh=split, in_specs=placed, out_specs=(rows, rows), check_vma=False)
```
